32 devices in a mesh: dp: 4 (over z), expert: 2 (over x), shard: 4 (over y, core).
Axes of the slice: x: 2, y: 2, z: 4, core: 2. Of those that a mesh axis runs over, the one named last changes fastest.
Arguments:
- activations: bfloat16 [2, 2, 2048, 256], P(None, 'expert', ('dp', 'shard')), may hold values from -6 to 6
- out_grads: bfloat16 [2, 2, 2048, 14336], P(None, 'expert', ('dp', 'shard')), may hold values from -0.25 to 0.25
- weights: float32 [2, 2, 256, 14336], P(None, 'expert', ('dp', 'shard')), may hold values from -4 to 4
- shadow: float32 [2, 2, 256, 14336], P(None, 'expert', ('dp', 'shard')), may hold values from -4 to 4
- counts: int32 [2, 32, 2], P(None, ('dp', 'expert', 'shard')), may hold values from 1 to 1024, as said below
Outputs:
- new_weights: float32 [2, 2, 256, 14336], P(None, 'expert', ('dp', 'shard'))
- new_shadow: float32 [2, 2, 256, 14336], P(None, 'expert', ('dp', 'shard'))
The draws below stay inside these ranges and needn't reach their ends.
Inputs may be any that keep to these rules, and one draw needn't show every extreme that they name: `counts`: loads differ between the experts of a layer.
All inputs are finite; a program needn't handle non-finite values.
Results may differ from the reference program's by a relative error of at most 0.0003.
Values sent between devices are 32-bit elements; how exact they have to be, the bound alone decides.
A program may use at most 128 MiB of HBM per device.

```python
import jax
import jax.numpy as jnp
from jax import lax

FF = 14336
ROWS = 256
TOK_DEV = 128
LAYERS = 2
EXPERTS = 2
TOKENS = 2048
DEVICES = 32


def draw_activations(key, part):
    base = jax.random.normal(key, (LAYERS, EXPERTS, TOKENS, ROWS), jnp.float32)
    return jnp.clip(base, -6.0, 6.0).astype(jnp.bfloat16)


def draw_out_grads(key, part):
    base = 0.03 * jax.random.normal(key, (LAYERS, EXPERTS, TOKENS, FF), jnp.float32)
    return jnp.clip(base, -0.25, 0.25).astype(jnp.bfloat16)


def draw_counts(key, part):
    ranges = jax.random.randint(jax.random.fold_in(key, 3), (LAYERS, 1, EXPERTS), 1, 9)
    raw = jax.random.randint(key, (LAYERS, DEVICES, EXPERTS), 0, 1 << 20)
    values = 1 + raw % (TOK_DEV * ranges)
    chosen_device = jax.random.randint(jax.random.fold_in(key, 5), (LAYERS, 1, 1), 0, DEVICES)
    chosen_expert = jax.random.randint(jax.random.fold_in(key, 6), (LAYERS, 1, 1), 0, EXPERTS)
    device_ids = jnp.arange(DEVICES, dtype=jnp.int32)[None, :, None]
    expert_ids = jnp.arange(EXPERTS, dtype=jnp.int32)[None, None, :]
    marked = (device_ids == chosen_device) & (expert_ids == chosen_expert)
    values = jnp.where(marked, 8 * TOK_DEV, values)
    return values.astype(jnp.int32)


def levels(key, dims, pieces, low, largest):
    level, own = 1.0, jax.random.fold_in(key, 6)
    for axis_at, parts in pieces:
        steps = jnp.exp(jax.random.uniform(jax.random.fold_in(own, axis_at), (parts,), jnp.float32, low / len(pieces), largest / len(pieces)))
        level = level * jnp.repeat(steps, dims[axis_at] // parts).reshape([-1 if axis == axis_at else 1 for axis in range(len(dims))])
    return level


def normal_values(stream_key, dims, spread, reach, pieces=(), held_as=jnp.bfloat16):
    drawn = spread * jax.random.normal(stream_key, dims, jnp.float32)
    if pieces:
        drawn = drawn * levels(stream_key, dims, pieces, -0.22, 0.18)
    return jnp.clip(drawn, -reach, reach).astype(held_as)


def setup_inputs(seed: int = 0) -> dict:
    streams_of = jax.random.split(jax.random.key(seed), 6)
    return {
        "activations": draw_activations(jax.random.fold_in(streams_of[5], 71), 0),
        "out_grads": draw_out_grads(jax.random.fold_in(streams_of[5], 71), 0),
        "weights": normal_values(streams_of[2], (LAYERS, EXPERTS, ROWS, FF), 0.5, 4.0, ((1, 2), (2, 16)), jnp.float32),
        "shadow": normal_values(streams_of[3], (LAYERS, EXPERTS, ROWS, FF), 0.5, 4.0, ((1, 2), (2, 16)), jnp.float32),
        "counts": draw_counts(jax.random.fold_in(streams_of[5], 71), 0),
    }


step_size = 0.5
clip_level = 1.0

def reference(activations, out_grads, weights, shadow, counts):
    totals = lax.optimization_barrier(jnp.sum(counts, axis=1, dtype=jnp.int32))
    all_weights = []
    all_shadow = []
    for layer_index in range(LAYERS):
        loads = totals[layer_index].astype(jnp.float32)
        mean_load = jnp.mean(loads)

        def update_one(item):
            inputs, cotangent, current, smooth, own_load = item
            summed = jnp.dot(inputs.T, cotangent, preferred_element_type=jnp.float32)
            numel = summed.shape[0] * summed.shape[1]
            root_mean = jnp.sqrt(jnp.sum(summed * summed) / numel)
            factor = step_size * (own_load / mean_load) * clip_level / jnp.maximum(root_mean, clip_level)
            updated = current - factor * summed
            beta = own_load / (own_load + mean_load)
            return (updated, smooth + beta * (updated - smooth))
        updated, smoothed = lax.map(update_one, (activations[layer_index], out_grads[layer_index], weights[layer_index], shadow[layer_index], loads))
        all_weights.append(updated)
        all_shadow.append(smoothed)
    return (jnp.stack(all_weights), jnp.stack(all_shadow))
```

```python
import functools

import jax
import jax.numpy as jnp
from jax import lax
from jax.experimental import pallas as pl
from jax.experimental.pallas import tpu as pltpu
from jax.sharding import PartitionSpec as P

step_size = 0.5
clip_level = 1.0
CORES = 2
SLOTS = 4
LAG = 5
HOP = 2
HOP_LATE = 4
AHEAD = 6
RING = 8
PIECES = 28
MESH = pl.DeviceIdType.MESH


def kernel(
    dims, acts, cot_hbm, cnt, out_ref, stat_ref,
    turned, rows_ref, cot, merged, from_y, from_z, from_zx, late_y, staged,
    squares, counted, seen, message, gathered,
    cot_sem, core_send, core_recv, y_send, y_recv, z_send, z_recv,
    zx_send, zx_recv, late_send, late_recv, cnt_send, cnt_recv, all_send, all_recv,
):
    line, experts, shards, layers, per_layer, width, rows, numel, period, lates = dims
    group = line * shards
    half = line * rows
    chunks = layers * per_layer
    z, e, s = lax.axis_index("dp"), lax.axis_index("expert"), lax.axis_index("shard")
    y, c = s // CORES, s % CORES
    me = z * shards + s
    core_peer = {"shard": y * CORES + (1 - c)}
    y_peer = {"shard": (1 - y) * CORES + c}
    own, other = y * half, (1 - y) * half

    def place(k):
        return k // per_layer, k % per_layer

    def columns(q):
        return pl.ds(pl.multiple_of(q * width, 128), width)

    def fetch(k):
        layer, q = place(k)
        return pltpu.make_async_copy(
            cot_hbm.at[layer, :, columns(q)], cot.at[k % RING], cot_sem.at[k % RING]
        )

    for k in range(min(AHEAD, chunks)):
        fetch(k).start()

    def group_peer(d):
        p = lax.rem(me + d, group)
        return p, {"dp": p // shards, "shard": p % shards}

    def remote(src, dst, send, recv, device):
        return pltpu.make_async_remote_copy(
            src_ref=src, dst_ref=dst, send_sem=send, recv_sem=recv,
            device_id=device, device_id_type=MESH,
        )

    barrier = pltpu.get_barrier_semaphore()
    for d in range(1, group):
        pl.semaphore_signal(barrier, inc=1, device_id=group_peer(d)[1], device_id_type=MESH)
    for d in range(1, experts):
        pl.semaphore_signal(
            barrier, inc=1, device_id={"expert": lax.rem(e + d, experts)}, device_id_type=MESH
        )

    for layer in range(layers):
        across = acts[layer].astype(jnp.float32).T
        for b in range(line):
            for h in range(shards // CORES):
                for core in range(CORES):
                    at = ((b * (shards // CORES) + h) * CORES + core) * rows
                    to = (h * line + b) * rows
                    turned[core, to:to + rows, :] = across[at:at + rows]
        for core in range(CORES):
            rows_ref[layer, core] = turned[core].astype(rows_ref.dtype)

    row = lax.broadcasted_iota(jnp.int32, counted.shape, 0)
    lane = lax.broadcasted_iota(jnp.int32, counted.shape, 1)
    tile = jnp.zeros(counted.shape, jnp.float32)
    for layer in range(layers):
        for p in range(experts):
            here = (row == layers + layer) & (lane == p)
            tile = jnp.where(here, cnt[layer, 0, p].astype(jnp.float32), tile)
    counted[...] = tile
    squares[...] = jnp.zeros_like(squares)

    pl.semaphore_wait(barrier, group + experts - 2)

    def count_copy(d, sender):
        return remote(
            counted, seen.at[sender], cnt_send.at[d], cnt_recv.at[sender],
            {"expert": lax.rem(e + d, experts)},
        )

    for d in range(1, experts):
        count_copy(d, e).start()

    def is_late(k):
        return (k % period == 1) & (k < period * lates)

    def when_chunk(k, body):
        pl.when((k >= 0) & (k < chunks))(lambda: body(k))

    def when_early(k, body):
        when_chunk(k, lambda k: pl.when(jnp.logical_not(is_late(k)))(lambda: body(k)))

    def when_late(k, body):
        when_chunk(k, lambda k: pl.when(is_late(k))(lambda: body(k)))

    def core_copy(k):
        return remote(
            staged.at[k % SLOTS], merged.at[k], core_send.at[k % SLOTS], core_recv.at[k], core_peer
        )

    def y_copy(k):
        return remote(
            merged.at[k, pl.ds(pl.multiple_of(other, 8), half)], from_y.at[k],
            y_send.at[k], y_recv.at[k], y_peer,
        )

    def late_copy(k):
        j = k // period
        return remote(
            merged.at[k, pl.ds(pl.multiple_of(other + z * rows, 8), rows)], late_y.at[j],
            late_send.at[j], late_recv.at[j], y_peer,
        )

    def product(k, core):
        layer, _ = place(k)
        return jnp.dot(
            rows_ref[layer, core], cot[k % RING], preferred_element_type=jnp.float32
        )

    def stage_partner(k):
        pl.when(k >= SLOTS)(lambda: core_copy(k - SLOTS).wait_send())
        fetch(k).wait()
        staged[k % SLOTS] = product(k, 1 - c)
        core_copy(k).start()

    def merge_core(k):
        core_copy(k).wait_recv()
        merged[k] = merged[k] + product(k, c)
        pl.when(jnp.logical_not(is_late(k)))(lambda: y_copy(k).start())

    def merge_y(k):
        y_copy(k).wait_recv()
        at = pl.ds(pl.multiple_of(own, 8), half)
        merged[k, at, :] = merged[k, at, :] + from_y[k]

    def block(k, base, b):
        return merged.at[k, pl.ds(pl.multiple_of(base + b * rows, 8), rows)]

    def z_copy(k, base, b, slot, device, extra):
        if extra:
            j = k // period
            return remote(
                block(k, base, b), from_zx.at[j, slot], zx_send.at[j, b], zx_recv.at[j, slot],
                device,
            )
        return remote(
            block(k, base, b), from_z.at[k, slot], z_send.at[k, b], z_recv.at[k, slot], device
        )

    def arrived(k, slot, extra):
        return from_zx[k // period, slot] if extra else from_z[k, slot]

    def add_arrived(k, base, b, slot, extra):
        z_copy(k, base, b, slot, {"dp": z}, extra).wait_recv()
        ref = block(k, base, b)
        ref[...] = ref[...] + arrived(k, slot, extra)

    def to_right(k, base, extra):
        for b in reversed(range(1, line)):
            @pl.when(z < b)
            def _():
                pl.when(z > 0)(lambda: add_arrived(k, base, b, b + 1, extra))
                z_copy(k, base, b, b + 1, {"dp": z + 1}, extra).start()

    def to_left(k, base, extra):
        for b in range(line - 1):
            @pl.when(z > b)
            def _():
                pl.when(z < line - 1)(lambda: add_arrived(k, base, b, b, extra))
                z_copy(k, base, b, b, {"dp": z - 1}, extra).start()

    def both_halves(one):
        def body(k):
            one(k, other, True)
            one(k, own, False)
        return body

    def own_half(one):
        return lambda k: one(k, own, False)

    def put(k, values):
        layer, q = place(k)
        out_ref[layer, :, columns(q)] = values
        squares[layer] = squares[layer] + values * values

    def gather_block(k, base, extra):
        pl.when(z > 0)(lambda: add_arrived(k, base, z, z + 1, extra))
        pl.when(z < line - 1)(lambda: add_arrived(k, base, z, z, extra))

    def finish_early(k):
        gather_block(k, own, False)
        put(k, block(k, own, z)[...])

    def finish_late(k):
        gather_block(k, other, True)
        late_copy(k).start()
        gather_block(k, own, False)

    back = line - 1 - z
    far = jnp.maximum(z, back)

    def step(t, _):
        pl.when(t + AHEAD < chunks)(lambda: fetch(t + AHEAD).start())
        when_chunk(t, stage_partner)
        when_chunk(t - 1, merge_core)
        when_late(t - 1 - HOP_LATE * z, both_halves(to_right))
        when_late(t - 1 - HOP_LATE * back, both_halves(to_left))
        when_late(t - 1 - HOP_LATE * far, finish_late)
        when_early(t - LAG, merge_y)
        when_early(t - LAG - HOP * z, own_half(to_right))
        when_early(t - LAG - HOP * back, own_half(to_left))
        when_early(t - LAG - HOP * far, finish_early)
        return 0

    steps = chunks + LAG + HOP * (line - 1)
    steps = max(steps, period * (lates - 1) + 3 + HOP_LATE * (line - 1))
    lax.fori_loop(0, steps, step, 0)

    def add_late(j, _):
        k = j * period + 1
        late_copy(k).wait_recv()
        put(k, block(k, own, z)[...] + late_y[j])
        return 0

    lax.fori_loop(0, lates, add_late, 0)

    totals = counted[...]
    for d in range(1, experts):
        sender = lax.rem(e + d, experts)
        count_copy(d, sender).wait_recv()
        totals = totals + seen[sender]
    for layer in range(layers):
        share = jnp.sum(jnp.sum(squares[layer], axis=0, keepdims=True), axis=1, keepdims=True)
        totals = jnp.where(row == layer, share, totals)
    message[...] = totals
    gathered[me] = totals

    def all_copy(d, sender):
        return remote(
            message, gathered.at[sender], all_send.at[d], all_recv.at[sender], group_peer(d)[1]
        )

    for d in range(1, group):
        all_copy(d, me).start()
    for d in range(1, group):
        all_copy(d, group_peer(d)[0]).wait_recv()
    total = gathered[0]
    for p in range(1, group):
        total = total + gathered[p]
    stats = jnp.zeros_like(total)
    for layer in range(layers):
        loads = total[layers + layer:layers + layer + 1, :]
        spot = lane[:1]
        own_load = jnp.sum(jnp.where(spot == e, loads, 0.0), axis=1, keepdims=True)
        mean_load = jnp.sum(jnp.where(spot < experts, loads, 0.0), axis=1, keepdims=True) / experts
        root_mean = jnp.sqrt(total[layer:layer + 1, :1] / numel)
        factor = (
            step_size * (own_load / mean_load) * clip_level / jnp.maximum(root_mean, clip_level)
        )
        beta = own_load / (own_load + mean_load)
        stats = jnp.where(row == layer, factor, stats)
        stats = jnp.where(row == layers + layer, beta, stats)
    stat_ref[...] = stats

    for d in range(1, group):
        all_copy(d, me).wait_send()
    for d in range(1, experts):
        count_copy(d, e).wait_send()
    for k in range(chunks - min(SLOTS, chunks), chunks):
        core_copy(k).wait_send()

    def drain(k, _):
        pl.when(jnp.logical_not(is_late(k)))(lambda: y_copy(k).wait_send())
        for b in range(line):
            pl.when(z != b)(lambda: z_copy(k, own, b, b, {"dp": z}, False).wait_send())
        return 0

    def drain_late(j, _):
        k = j * period + 1
        late_copy(k).wait_send()
        for b in range(line):
            pl.when(z != b)(lambda: z_copy(k, other, b, b, {"dp": z}, True).wait_send())
        return 0

    lax.fori_loop(0, chunks, drain, 0)
    lax.fori_loop(0, lates, drain_late, 0)


def on_device(sizes, activations, out_grads, weights, shadow, counts):
    line, experts, shards = sizes
    layers, _, tokens, all_rows = activations.shape
    ff, rows = out_grads.shape[3], weights.shape[2]
    assert shards == 2 * CORES and 2 * layers <= 8
    units = ff // 128
    per_layer = next(
        p for p in range(PIECES, units + 1) if units % p == 0 and units // p % 2 == 0
    )
    width = ff // per_layer
    chunks = layers * per_layer
    half = line * rows
    group = line * shards
    period = max(2, 2 * (line - 1))
    lates = chunks // period
    f32 = jnp.float32
    dma = pltpu.SemaphoreType.DMA
    vmem = pl.BlockSpec(memory_space=pltpu.VMEM)
    hbm = pl.BlockSpec(memory_space=pltpu.HBM)
    dims = (line, experts, shards, layers, per_layer, width, rows, all_rows * ff, period, lates)
    summed, stats = pl.pallas_call(
        functools.partial(kernel, dims),
        out_shape=(
            jax.ShapeDtypeStruct((layers, rows, ff), f32), jax.ShapeDtypeStruct((8, 128), f32)
        ),
        in_specs=[vmem, hbm, pl.BlockSpec(memory_space=pltpu.SMEM)],
        out_specs=(vmem, vmem),
        scratch_shapes=[
            pltpu.VMEM((CORES, 2 * half, tokens), f32),
            pltpu.VMEM((layers, CORES, 2 * half, tokens), activations.dtype),
            pltpu.VMEM((RING, tokens, width), out_grads.dtype),
            pltpu.VMEM((chunks, 2 * half, width), f32),
            pltpu.VMEM((chunks, half, width), f32),
            pltpu.VMEM((chunks, line + 1, rows, width), f32),
            pltpu.VMEM((lates, line + 1, rows, width), f32),
            pltpu.VMEM((lates, rows, width), f32),
            pltpu.VMEM((SLOTS, 2 * half, width), f32),
            pltpu.VMEM((layers, rows, width), f32),
            pltpu.VMEM((8, 128), f32),
            pltpu.VMEM((experts, 8, 128), f32),
            pltpu.VMEM((8, 128), f32),
            pltpu.VMEM((group, 8, 128), f32),
            dma((RING,)),
            dma((SLOTS,)), dma((chunks,)), dma((chunks,)), dma((chunks,)),
            dma((chunks, line)), dma((chunks, line + 1)),
            dma((lates, line)), dma((lates, line + 1)),
            dma((lates,)), dma((lates,)), dma((experts,)), dma((experts,)),
            dma((group,)), dma((group,)),
        ],
        compiler_params=pltpu.CompilerParams(
            collective_id=0, has_side_effects=True, vmem_limit_bytes=46 * 1024 * 1024
        ),
        name="reduce_gradient",
    )(activations[:, 0], out_grads[:, 0], counts)
    factor = stats[:layers, 0][:, None, None]
    beta = stats[layers:2 * layers, 0][:, None, None]
    updated = weights[:, 0] - factor * summed
    previous = shadow[:, 0]
    return updated[:, None], (previous + beta * (updated - previous))[:, None]


def solution(mesh):
    rows = P(None, "expert", ("dp", "shard"), None)
    in_specs = (rows, rows, rows, rows, P(None, ("dp", "expert", "shard"), None))
    sizes = tuple(mesh.shape[a] for a in ("dp", "expert", "shard"))
    return jax.shard_map(
        functools.partial(on_device, sizes), mesh=mesh, in_specs=in_specs,
        out_specs=(rows, rows), check_vma=False,
    )
```

```python
import functools

import jax
import jax.numpy as jnp
from jax import lax
from jax.experimental import pallas as pl
from jax.experimental.pallas import tpu as pltpu
from jax.sharding import PartitionSpec as P

step_size = 0.5
clip_level = 1.0
CORES = 2
SLOTS = 4
LAG = 6
HOP = 3
HOP_LATE = 3
TAIL = 6
AHEAD = 6
RING = 8
CUT = 0
FEWER = 0
PIECES = 28
MESH = pl.DeviceIdType.MESH


def kernel(
    dims, act_hbm, cot_hbm, cnt_hbm, out_ref, stat_ref,
    acts, cnt, turned, rows_ref, cot, merged, from_y, from_z, from_zx, late_y, staged,
    squares, counted, seen, message, gathered,
    act_sem, cnt_sem, cot_sem, core_send, core_recv, y_send, y_recv, tail_send, tail_recv, z_send, z_recv,
    zx_send, zx_recv, late_send, late_recv, cnt_send, cnt_recv, all_send, all_recv,
):
    line, experts, shards, layers, per_layer, width, rows, numel, period, lates, ring, late_ring, y_ring = dims
    group = line * shards
    half = line * rows
    chunks = layers * per_layer
    first_tail = chunks - TAIL
    z, e, s = lax.axis_index("dp"), lax.axis_index("expert"), lax.axis_index("shard")
    y, c = s // CORES, s % CORES
    me = z * shards + s
    core_peer = {"shard": y * CORES + (1 - c)}
    y_peer = {"shard": (1 - y) * CORES + c}
    own, other = y * half, (1 - y) * half

    def place(k):
        return k // per_layer, k % per_layer

    def columns(q):
        return pl.ds(pl.multiple_of(q * width, 128), width)

    def fetch(k):
        layer, q = place(k)
        return pltpu.make_async_copy(
            cot_hbm.at[layer, :, columns(q)], cot.at[k % RING], cot_sem.at[k % RING]
        )

    act_copy = pltpu.make_async_copy(act_hbm, acts, act_sem)
    cnt_fetch = pltpu.make_async_copy(cnt_hbm, cnt, cnt_sem)
    act_copy.start()
    fetch(0).start()

    def group_peer(d):
        p = lax.rem(me + d, group)
        return p, {"dp": p // shards, "shard": p % shards}

    def remote(src, dst, send, recv, device):
        return pltpu.make_async_remote_copy(
            src_ref=src, dst_ref=dst, send_sem=send, recv_sem=recv,
            device_id=device, device_id_type=MESH,
        )

    barrier = pltpu.get_barrier_semaphore()
    for d in range(1, group):
        pl.semaphore_signal(barrier, inc=1, device_id=group_peer(d)[1], device_id_type=MESH)
    for d in range(1, experts):
        pl.semaphore_signal(
            barrier, inc=1, device_id={"expert": lax.rem(e + d, experts)}, device_id_type=MESH
        )

    for k in range(1, min(AHEAD, chunks)):
        fetch(k).start()
    cnt_fetch.start()

    def turn(layer):
        across = acts[layer].astype(jnp.float32).T
        for b in range(line):
            for h in range(shards // CORES):
                for core in range(CORES):
                    at = ((b * (shards // CORES) + h) * CORES + core) * rows
                    to = (h * line + b) * rows
                    turned[core, to:to + rows, :] = across[at:at + rows]
        for core in range(CORES):
            rows_ref[layer, core] = turned[core].astype(rows_ref.dtype)

    act_copy.wait()
    turn(0)
    pl.semaphore_wait(barrier, group + experts - 2)

    row = lax.broadcasted_iota(jnp.int32, counted.shape, 0)
    lane = lax.broadcasted_iota(jnp.int32, counted.shape, 1)

    def count_copy(d, sender):
        return remote(
            counted, seen.at[sender], cnt_send.at[d], cnt_recv.at[sender],
            {"expert": lax.rem(e + d, experts)},
        )

    def prepare():
        for layer in range(1, layers):
            turn(layer)
        cnt_fetch.wait()
        tile = jnp.zeros(counted.shape, jnp.float32)
        for layer in range(layers):
            for p in range(experts):
                here = (row == layers + layer) & (lane == p)
                tile = jnp.where(here, cnt[layer, 0, p].astype(jnp.float32), tile)
        counted[...] = tile
        squares[...] = jnp.zeros_like(squares)
        for d in range(1, experts):
            count_copy(d, e).start()

    def is_late(k):
        return (k % period == 1) & (k < period * lates)

    def late_chunk(j):
        return j * period + 1

    def when_chunk(k, body):
        pl.when((k >= 0) & (k < chunks))(lambda: body(k))

    def when_early(k, body):
        when_chunk(k, lambda k: pl.when(jnp.logical_not(is_late(k)))(lambda: body(k)))

    def when_chain(k, body):
        when_early(k, lambda k: pl.when(k < first_tail)(lambda: body(k)))

    def when_tail(k, body):
        pl.when((k >= first_tail) & (k < chunks))(lambda: body(k))

    def when_late(k, body):
        when_chunk(k, lambda k: pl.when(is_late(k))(lambda: body(k)))

    def core_copy(k):
        return remote(
            staged.at[k % SLOTS], merged.at[k], core_send.at[k % SLOTS], core_recv.at[k % SLOTS], core_peer
        )

    def y_copy(k):
        return remote(
            merged.at[k, pl.ds(pl.multiple_of(other, 8), half)], from_y.at[k],
            y_send.at[k % y_ring], y_recv.at[k % y_ring], y_peer,
        )

    def late_copy(k):
        j = k // period
        return remote(
            merged.at[k, pl.ds(pl.multiple_of(other + z * rows, 8), rows)], late_y.at[j],
            late_send.at[j], late_recv.at[j], y_peer,
        )

    def product(k, core):
        layer, _ = place(k)
        return jnp.dot(
            rows_ref[layer, core], cot[k % RING], preferred_element_type=jnp.float32
        )

    def stage_partner(k):
        pl.when(k >= SLOTS)(lambda: core_copy(k - SLOTS).wait_send())
        fetch(k).wait()
        staged[k % SLOTS] = product(k, 1 - c)
        core_copy(k).start()

    def merge_core(k):
        core_copy(k).wait_recv()
        merged[k] = merged[k] + product(k, c)
        when_chain(k, lambda k: y_copy(k).start())
        when_tail(k, lambda k: other_blocks(lambda b: tail_copy(k, b).start()))

    def tail_copy(k, b):
        i = k - first_tail
        at = pl.ds(pl.multiple_of(other + b * rows, 8), rows)
        return remote(
            merged.at[k, at], from_y.at[k, b * rows:(b + 1) * rows],
            tail_send.at[i, b], tail_recv.at[i, b], y_peer,
        )

    def other_blocks(body):
        for b in range(line):
            pl.when(z != b)(lambda: body(b))

    def own_block(body):
        for b in range(line):
            pl.when(z == b)(lambda: body(b))

    def merge_y(k):
        y_copy(k).wait_recv()
        at = pl.ds(pl.multiple_of(own, 8), half)
        merged[k, at, :] = merged[k, at, :] + from_y[k]

    def merge_block(k, b):
        tail_copy(k, b).wait_recv()
        at = pl.ds(pl.multiple_of(own + b * rows, 8), rows)
        merged[k, at, :] = merged[k, at, :] + from_y[k, b * rows:(b + 1) * rows, :]

    def merge_tail(k):
        other_blocks(lambda b: merge_block(k, b))

    def block(k, base, b):
        return merged.at[k, pl.ds(pl.multiple_of(base + b * rows, 8), rows)]

    def z_copy(k, base, b, slot, device, late):
        if late is None:
            return remote(
                block(k, base, b), from_z.at[k, slot], z_send.at[k % ring, b],
                z_recv.at[k % ring, slot], device,
            )
        j = k // period
        n = late * (line + 1) + slot
        return remote(
            block(k, base, b), from_zx.at[j, n], zx_send.at[j % late_ring, late * line + b],
            zx_recv.at[j % late_ring, n], device,
        )

    def arrived(k, slot, late):
        if late is None:
            return from_z[k, slot]
        return from_zx[k // period, late * (line + 1) + slot]

    def add_arrived(k, base, b, slot, late):
        z_copy(k, base, b, slot, {"dp": z}, late).wait_recv()
        ref = block(k, base, b)
        ref[...] = ref[...] + arrived(k, slot, late)

    def send_right(k, base, b, late):
        @pl.when(z < b)
        def _():
            pl.when(z > 0)(lambda: add_arrived(k, base, b, b + 1, late))
            z_copy(k, base, b, b + 1, {"dp": z + 1}, late).start()

    def send_left(k, base, b, late):
        @pl.when(z > b)
        def _():
            pl.when(z < line - 1)(lambda: add_arrived(k, base, b, b, late))
            z_copy(k, base, b, b, {"dp": z - 1}, late).start()

    def to_right(k, base, late):
        for b in reversed(range(1, line)):
            send_right(k, base, b, late)

    def to_left(k, base, late):
        for b in range(line - 1):
            send_left(k, base, b, late)

    def far_right(k):
        for b in reversed(range(2, line)):
            pl.when(z + 1 < b)(lambda: send_right(k, own, b, None))

    def far_left(k):
        for b in range(line - 2):
            pl.when(z - 1 > b)(lambda: send_left(k, own, b, None))

    def near_right(k, _):
        for b in range(1, line):
            pl.when(z + 1 == b)(lambda: send_right(k, own, b, None))

    def near_left(k, _):
        for b in range(line - 1):
            pl.when(z - 1 == b)(lambda: send_left(k, own, b, None))

    def both_halves(one):
        def body(k):
            one(k, other, 0)
            one(k, own, 1)
        return body

    def own_half(one):
        return lambda k: one(k, own, None)

    def put(k, values):
        layer, q = place(k)
        out_ref[layer, :, columns(q)] = values
        squares[layer] = squares[layer] + values * values

    def gather_block(k, base, late):
        pl.when(z > 0)(lambda: add_arrived(k, base, z, z + 1, late))
        pl.when(z < line - 1)(lambda: add_arrived(k, base, z, z, late))

    def finish_early(k):
        gather_block(k, own, None)
        put(k, block(k, own, z)[...])

    def finish_tail(k, _):
        own_block(lambda b: merge_block(k, b))
        finish_early(k)

    def finish_late(k):
        gather_block(k, other, 0)
        gather_block(k, own, 1)

    back = line - 1 - z
    far = jnp.maximum(z, back)

    def on_tail(body):
        return lambda: lax.fori_loop(first_tail, chunks, body, None)

    def step(t, _):
        pl.when(t + AHEAD < chunks)(lambda: fetch(t + AHEAD).start())
        when_chunk(t, stage_partner)
        when_chunk(t - 1, merge_core)
        when_late(t - 1 - HOP_LATE * z, both_halves(to_right))
        when_late(t - 1 - HOP_LATE * back, both_halves(to_left))
        when_late(t - 1 - HOP_LATE * far, finish_late)
        pl.when(t == 2)(prepare)
        when_chain(t - LAG, merge_y)
        when_tail(t - LAG, merge_tail)
        when_chain(t - LAG - HOP * z, own_half(to_right))
        when_chain(t - LAG - HOP * back, own_half(to_left))
        when_chain(t - LAG - HOP * far, finish_early)
        when_tail(t - LAG - HOP * z, far_right)
        when_tail(t - LAG - HOP * back, far_left)
        pl.when(t == chunks - 1 + LAG + HOP * z)(on_tail(near_right))
        pl.when(t == chunks - 1 + LAG + HOP * back)(on_tail(near_left))
        pl.when(t == start_late)(send_lates)
        when_chain(t - LAG - 1, drain_y)
        when_late(t - late_behind, drain_late)
        when_chain(t - behind, drain_z)
        return 0

    late_end = late_chunk(lates - 1) + 1 + HOP_LATE * (line - 1)
    start_late = max(chunks, late_end)
    behind = LAG + HOP * (line - 1) + 3
    late_behind = HOP_LATE * (line - 1) + 3
    steps = max(chunks + LAG + HOP * (line - 1), start_late + 1)

    def send_late(j, _):
        late_copy(late_chunk(j)).start()

    def send_own(k, _):
        own_block(lambda b: tail_copy(k, b).start())

    def send_lates():
        lax.fori_loop(0, lates, send_late, None)
        lax.fori_loop(first_tail, chunks, send_own, None)

    def drain_y(k):
        y_copy(k).wait_send()

    def drain_z(k):
        for b in range(line):
            pl.when(z != b)(lambda: z_copy(k, own, b, b, {"dp": z}, None).wait_send())

    def drain_late(k):
        for b in range(line):
            pl.when(z != b)(lambda: z_copy(k, other, b, b, {"dp": z}, 0).wait_send())
            pl.when(z != b)(lambda: z_copy(k, own, b, b, {"dp": z}, 1).wait_send())

    lax.fori_loop(0, steps, step, 0)

    def add_late(j, _):
        k = late_chunk(j)
        late_copy(k).wait_recv()
        put(k, block(k, own, z)[...] + late_y[j])
        return 0

    lax.fori_loop(0, lates, add_late, 0)
    lax.fori_loop(first_tail, chunks, finish_tail, None)

    totals = counted[...]
    for d in range(1, experts):
        sender = lax.rem(e + d, experts)
        count_copy(d, sender).wait_recv()
        totals = totals + seen[sender]
    for layer in range(layers):
        share = jnp.sum(jnp.sum(squares[layer], axis=0, keepdims=True), axis=1, keepdims=True)
        totals = jnp.where(row == layer, share, totals)
    message[...] = totals
    gathered[me] = totals

    def all_copy(d, sender):
        return remote(
            message, gathered.at[sender], all_send.at[d], all_recv.at[sender], group_peer(d)[1]
        )

    for d in range(1, group):
        all_copy(d, me).start()
    def drain_rest(k, _):
        drain_z(k)
        for b in range(line):
            tail_copy(k, b).wait_send()

    for k in range(chunks - min(SLOTS, chunks), chunks):
        core_copy(k).wait_send()
    lax.fori_loop(
        steps - behind, first_tail, lambda k, _: when_chain(k, drain_z), None
    )
    lax.fori_loop(first_tail, chunks, drain_rest, None)
    lax.fori_loop(
        0, lates, lambda j, _: late_copy(late_chunk(j)).wait_send(), None
    )

    for d in range(1, group):
        all_copy(d, group_peer(d)[0]).wait_recv()
    total = gathered[0]
    for p in range(1, group):
        total = total + gathered[p]
    stats = jnp.zeros_like(total)
    for layer in range(layers):
        loads = total[layers + layer:layers + layer + 1, :]
        spot = lane[:1]
        own_load = jnp.sum(jnp.where(spot == e, loads, 0.0), axis=1, keepdims=True)
        mean_load = jnp.sum(jnp.where(spot < experts, loads, 0.0), axis=1, keepdims=True) / experts
        root_mean = jnp.sqrt(total[layer:layer + 1, :1] / numel)
        factor = (
            step_size * (own_load / mean_load) * clip_level / jnp.maximum(root_mean, clip_level)
        )
        beta = own_load / (own_load + mean_load)
        stats = jnp.where(row == layer, factor, stats)
        stats = jnp.where(row == layers + layer, beta, stats)
    stat_ref[...] = stats

    for d in range(1, group):
        all_copy(d, me).wait_send()
    for d in range(1, experts):
        count_copy(d, e).wait_send()


def on_device(sizes, activations, out_grads, weights, shadow, counts):
    line, experts, shards = sizes
    layers, _, tokens, all_rows = activations.shape
    ff, rows = out_grads.shape[3], weights.shape[2]
    assert shards == 2 * CORES and 2 * layers <= 8
    units = ff // 128
    per_layer = next(
        p for p in range(PIECES, units + 1) if units % p == 0 and units // p % 2 == 0
    )
    width = ff // per_layer
    chunks = layers * per_layer
    half = line * rows
    group = line * shards
    period = max(2, 2 * (line - 1))
    lates = chunks // period - FEWER
    period = max(2, period - CUT)
    ring = HOP * (line - 1) + HOP + 4
    y_ring = 2 * LAG + 2
    assert (lates - 1) * period + 1 < chunks - TAIL
    late_ring = min(lates, -(-(HOP_LATE * (line - 1) + HOP + 6) // period))
    f32 = jnp.float32
    dma = pltpu.SemaphoreType.DMA
    vmem = pl.BlockSpec(memory_space=pltpu.VMEM)
    hbm = pl.BlockSpec(memory_space=pltpu.HBM)
    dims = (
        line, experts, shards, layers, per_layer, width, rows, all_rows * ff, period, lates, ring,
        late_ring, y_ring,
    )
    summed, stats = pl.pallas_call(
        functools.partial(kernel, dims),
        out_shape=(
            jax.ShapeDtypeStruct((layers, rows, ff), f32), jax.ShapeDtypeStruct((8, 128), f32)
        ),
        in_specs=[hbm] * 3,
        out_specs=(vmem, vmem),
        scratch_shapes=[
            pltpu.VMEM((layers, tokens, all_rows), activations.dtype),
            pltpu.SMEM((layers, 1, experts), jnp.int32),
            pltpu.VMEM((CORES, 2 * half, tokens), f32),
            pltpu.VMEM((layers, CORES, 2 * half, tokens), activations.dtype),
            pltpu.VMEM((RING, tokens, width), out_grads.dtype),
            pltpu.VMEM((chunks, 2 * half, width), f32),
            pltpu.VMEM((chunks, half, width), f32),
            pltpu.VMEM((chunks, line + 1, rows, width), f32),
            pltpu.VMEM((lates, 2 * (line + 1), rows, width), f32),
            pltpu.VMEM((lates, rows, width), f32),
            pltpu.VMEM((SLOTS, 2 * half, width), f32),
            pltpu.VMEM((layers, rows, width), f32),
            pltpu.VMEM((8, 128), f32),
            pltpu.VMEM((experts, 8, 128), f32),
            pltpu.VMEM((8, 128), f32),
            pltpu.VMEM((group, 8, 128), f32),
            dma, dma, dma((RING,)),
            dma((SLOTS,)), dma((SLOTS,)), dma((y_ring,)), dma((y_ring,)),
            dma((TAIL, line)), dma((TAIL, line)),
            dma((ring, line)), dma((ring, line + 1)),
            dma((late_ring, 2 * line)), dma((late_ring, 2 * (line + 1))),
            dma((lates,)), dma((lates,)), dma((experts,)), dma((experts,)),
            dma((group,)), dma((group,)),
        ],
        compiler_params=pltpu.CompilerParams(
            collective_id=0, has_side_effects=True, vmem_limit_bytes=46 * 1024 * 1024
        ),
        name="reduce_gradient",
    )(
        pltpu.with_memory_space_constraint(activations[:, 0], pltpu.HBM), out_grads[:, 0],
        pltpu.with_memory_space_constraint(counts, pltpu.HBM),
    )
    factor = stats[:layers, 0][:, None, None]
    beta = stats[layers:2 * layers, 0][:, None, None]
    updated = weights[:, 0] - factor * summed
    previous = shadow[:, 0]
    return updated[:, None], (previous + beta * (updated - previous))[:, None]


def solution(mesh):
    rows = P(None, "expert", ("dp", "shard"), None)
    in_specs = (rows, rows, rows, rows, P(None, ("dp", "expert", "shard"), None))
    sizes = tuple(mesh.shape[a] for a in ("dp", "expert", "shard"))
    return jax.shard_map(
        functools.partial(on_device, sizes), mesh=mesh, in_specs=in_specs,
        out_specs=(rows, rows), check_vma=False,
    )
```

```python
import functools

import jax
import jax.numpy as jnp
from jax import lax
from jax.experimental import pallas as pl
from jax.experimental.pallas import tpu as pltpu
from jax.sharding import PartitionSpec as P

step_size = 0.5
clip_level = 1.0
CORES = 2
SLOTS = 4
LAG = 6
HOP = 3
HOP_LATE = 3
TAIL = 6
AHEAD = 6
RING = 8
CUT = 0
FEWER = 0
PIECES = 28
MESH = pl.DeviceIdType.MESH


def kernel(
    dims, act_hbm, cot_hbm, cnt_hbm, out_ref, stat_ref,
    acts, cnt, turned, rows_ref, cot, merged, from_y, from_z, from_zx, late_y, staged,
    squares, counted, seen, message, gathered,
    act_sem, cnt_sem, cot_sem, core_send, core_recv, y_send, y_recv, tail_send, tail_recv, z_send, z_recv,
    zx_send, zx_recv, late_send, late_recv, cnt_send, cnt_recv, all_send, all_recv,
):
    line, experts, shards, layers, per_layer, width, rows, numel, period, lates, ring, late_ring, y_ring = dims
    group = line * shards
    half = line * rows
    chunks = layers * per_layer
    first_tail = chunks - TAIL
    z, e, s = lax.axis_index("dp"), lax.axis_index("expert"), lax.axis_index("shard")
    y, c = s // CORES, s % CORES
    me = z * shards + s
    core_peer = {"shard": y * CORES + (1 - c)}
    y_peer = {"shard": (1 - y) * CORES + c}
    own, other = y * half, (1 - y) * half

    def place(k):
        return k // per_layer, k % per_layer

    def columns(q):
        return pl.ds(pl.multiple_of(q * width, 128), width)

    def fetch(k):
        layer, q = place(k)
        return pltpu.make_async_copy(
            cot_hbm.at[layer, :, columns(q)], cot.at[k % RING], cot_sem.at[k % RING]
        )

    act_copy = pltpu.make_async_copy(act_hbm, acts, act_sem)
    cnt_fetch = pltpu.make_async_copy(cnt_hbm, cnt, cnt_sem)
    act_copy.start()
    fetch(0).start()

    def group_peer(d):
        p = lax.rem(me + d, group)
        return p, {"dp": p // shards, "shard": p % shards}

    def remote(src, dst, send, recv, device):
        return pltpu.make_async_remote_copy(
            src_ref=src, dst_ref=dst, send_sem=send, recv_sem=recv,
            device_id=device, device_id_type=MESH,
        )

    barrier = pltpu.get_barrier_semaphore()
    def greet(device):
        pl.semaphore_signal(barrier, inc=1, device_id=device, device_id_type=MESH)

    greet(core_peer)
    greet(y_peer)
    pl.when(z > 0)(lambda: greet({"dp": z - 1}))
    pl.when(z < line - 1)(lambda: greet({"dp": z + 1}))
    for d in range(1, experts):
        greet({"expert": lax.rem(e + d, experts)})
    for k in range(1, min(AHEAD, chunks)):
        fetch(k).start()
    cnt_fetch.start()

    def turn(layer):
        across = acts[layer].astype(jnp.float32).T
        for b in range(line):
            for h in range(shards // CORES):
                for core in range(CORES):
                    at = ((b * (shards // CORES) + h) * CORES + core) * rows
                    to = (h * line + b) * rows
                    turned[core, to:to + rows, :] = across[at:at + rows]
        for core in range(CORES):
            rows_ref[layer, core] = turned[core].astype(rows_ref.dtype)

    act_copy.wait()
    turn(0)
    ends = (z == 0).astype(jnp.int32) + (z == line - 1).astype(jnp.int32)
    pl.semaphore_wait(barrier, experts + 3 - ends)

    row = lax.broadcasted_iota(jnp.int32, counted.shape, 0)
    lane = lax.broadcasted_iota(jnp.int32, counted.shape, 1)

    def count_copy(d, sender):
        return remote(
            counted, seen.at[sender], cnt_send.at[d], cnt_recv.at[sender],
            {"expert": lax.rem(e + d, experts)},
        )

    def prepare():
        for layer in range(1, layers):
            turn(layer)
        cnt_fetch.wait()
        tile = jnp.zeros(counted.shape, jnp.float32)
        for layer in range(layers):
            for p in range(experts):
                here = (row == layers + layer) & (lane == p)
                tile = jnp.where(here, cnt[layer, 0, p].astype(jnp.float32), tile)
        counted[...] = tile
        squares[...] = jnp.zeros_like(squares)
        for d in range(1, experts):
            count_copy(d, e).start()

    def is_late(k):
        return (k % period == 1) & (k < period * lates)

    def late_chunk(j):
        return j * period + 1

    def when_chunk(k, body):
        pl.when((k >= 0) & (k < chunks))(lambda: body(k))

    def when_early(k, body):
        when_chunk(k, lambda k: pl.when(jnp.logical_not(is_late(k)))(lambda: body(k)))

    def when_chain(k, body):
        when_early(k, lambda k: pl.when(k < first_tail)(lambda: body(k)))

    def when_tail(k, body):
        pl.when((k >= first_tail) & (k < chunks))(lambda: body(k))

    def when_late(k, body):
        when_chunk(k, lambda k: pl.when(is_late(k))(lambda: body(k)))

    def core_copy(k):
        return remote(
            staged.at[k % SLOTS], merged.at[k], core_send.at[k % SLOTS], core_recv.at[k % SLOTS], core_peer
        )

    def y_copy(k):
        return remote(
            merged.at[k, pl.ds(pl.multiple_of(other, 8), half)], from_y.at[k],
            y_send.at[k % y_ring], y_recv.at[k % y_ring], y_peer,
        )

    def late_copy(k):
        j = k // period
        return remote(
            merged.at[k, pl.ds(pl.multiple_of(other + z * rows, 8), rows)], late_y.at[j],
            late_send, late_recv, y_peer,
        )

    def product(k, core):
        layer, _ = place(k)
        return jnp.dot(
            rows_ref[layer, core], cot[k % RING], preferred_element_type=jnp.float32
        )

    def stage_partner(k):
        pl.when(k >= SLOTS)(lambda: core_copy(k - SLOTS).wait_send())
        fetch(k).wait()
        staged[k % SLOTS] = product(k, 1 - c)
        core_copy(k).start()

    def merge_core(k):
        core_copy(k).wait_recv()
        merged[k] = merged[k] + product(k, c)
        when_chain(k, lambda k: y_copy(k).start())
        when_tail(k, lambda k: other_blocks(lambda b: tail_copy(k, b).start()))

    def tail_copy(k, b):
        i = k - first_tail
        at = pl.ds(pl.multiple_of(other + b * rows, 8), rows)
        return remote(
            merged.at[k, at], from_y.at[k, b * rows:(b + 1) * rows],
            tail_send.at[i], tail_recv.at[i, b], y_peer,
        )

    def other_blocks(body):
        for b in range(line):
            pl.when(z != b)(lambda: body(b))

    def own_block(body):
        for b in range(line):
            pl.when(z == b)(lambda: body(b))

    def merge_y(k):
        y_copy(k).wait_recv()
        at = pl.ds(pl.multiple_of(own, 8), half)
        merged[k, at, :] = merged[k, at, :] + from_y[k]

    def merge_block(k, b):
        tail_copy(k, b).wait_recv()
        at = pl.ds(pl.multiple_of(own + b * rows, 8), rows)
        merged[k, at, :] = merged[k, at, :] + from_y[k, b * rows:(b + 1) * rows, :]

    def merge_tail(k):
        other_blocks(lambda b: merge_block(k, b))

    def block(k, base, b):
        return merged.at[k, pl.ds(pl.multiple_of(base + b * rows, 8), rows)]

    def z_copy(k, base, b, slot, device, late):
        if late is None:
            return remote(
                block(k, base, b), from_z.at[k, slot], z_send.at[k % ring],
                z_recv.at[k % ring, slot], device,
            )
        j = k // period
        n = late * (line + 1) + slot
        return remote(
            block(k, base, b), from_zx.at[j, n], zx_send.at[j % late_ring],
            zx_recv.at[j % late_ring, n], device,
        )

    def arrived(k, slot, late):
        if late is None:
            return from_z[k, slot]
        return from_zx[k // period, late * (line + 1) + slot]

    def add_arrived(k, base, b, slot, late):
        z_copy(k, base, b, slot, {"dp": z}, late).wait_recv()
        ref = block(k, base, b)
        ref[...] = ref[...] + arrived(k, slot, late)

    def send_right(k, base, b, late):
        @pl.when(z < b)
        def _():
            pl.when(z > 0)(lambda: add_arrived(k, base, b, b + 1, late))
            z_copy(k, base, b, b + 1, {"dp": z + 1}, late).start()

    def send_left(k, base, b, late):
        @pl.when(z > b)
        def _():
            pl.when(z < line - 1)(lambda: add_arrived(k, base, b, b, late))
            z_copy(k, base, b, b, {"dp": z - 1}, late).start()

    def to_right(k, base, late):
        for b in reversed(range(1, line)):
            send_right(k, base, b, late)

    def to_left(k, base, late):
        for b in range(line - 1):
            send_left(k, base, b, late)

    def far_right(k):
        for b in reversed(range(2, line)):
            pl.when(z + 1 < b)(lambda: send_right(k, own, b, None))

    def far_left(k):
        for b in range(line - 2):
            pl.when(z - 1 > b)(lambda: send_left(k, own, b, None))

    def near_right(k, _):
        for b in range(1, line):
            pl.when(z + 1 == b)(lambda: send_right(k, own, b, None))

    def near_left(k, _):
        for b in range(line - 1):
            pl.when(z - 1 == b)(lambda: send_left(k, own, b, None))

    def both_halves(one):
        def body(k):
            one(k, other, 0)
            one(k, own, 1)
        return body

    def own_half(one):
        return lambda k: one(k, own, None)

    def put(k, values):
        layer, q = place(k)
        out_ref[layer, :, columns(q)] = values
        squares[layer] = squares[layer] + values * values

    def gather_block(k, base, late):
        pl.when(z > 0)(lambda: add_arrived(k, base, z, z + 1, late))
        pl.when(z < line - 1)(lambda: add_arrived(k, base, z, z, late))

    def finish_early(k):
        gather_block(k, own, None)
        put(k, block(k, own, z)[...])

    def finish_tail(k, _):
        own_block(lambda b: merge_block(k, b))
        finish_early(k)

    def finish_late(k):
        gather_block(k, other, 0)
        gather_block(k, own, 1)

    back = line - 1 - z
    far = jnp.maximum(z, back)

    def on_tail(body):
        return lambda: lax.fori_loop(first_tail, chunks, body, None)

    def step(t, _):
        pl.when(t + AHEAD < chunks)(lambda: fetch(t + AHEAD).start())
        when_chunk(t, stage_partner)
        when_chunk(t - 1, merge_core)
        when_late(t - 1 - HOP_LATE * z, both_halves(to_right))
        when_late(t - 1 - HOP_LATE * back, both_halves(to_left))
        when_late(t - 1 - HOP_LATE * far, finish_late)
        pl.when(t == 2)(prepare)
        when_chain(t - LAG, merge_y)
        when_tail(t - LAG, merge_tail)
        when_chain(t - LAG - HOP * z, own_half(to_right))
        when_chain(t - LAG - HOP * back, own_half(to_left))
        when_chain(t - LAG - HOP * far, finish_early)
        when_tail(t - LAG - HOP * z, far_right)
        when_tail(t - LAG - HOP * back, far_left)
        pl.when(t == chunks - 1 + LAG + HOP * z)(on_tail(near_right))
        pl.when(t == chunks - 1 + LAG + HOP * back)(on_tail(near_left))
        pl.when(t == start_late)(send_lates)
        when_chain(t - LAG - 1, drain_y)
        when_late(t - late_behind, drain_late)
        when_chain(t - behind, drain_z)
        return 0

    late_end = late_chunk(lates - 1) + 1 + HOP_LATE * (line - 1)
    start_late = max(chunks, late_end)
    behind = LAG + HOP * (line - 1) + 3
    late_behind = HOP_LATE * (line - 1) + 3
    steps = max(chunks + LAG + HOP * (line - 1), start_late + 1)

    def send_late(j, _):
        late_copy(late_chunk(j)).start()

    def send_own(k, _):
        own_block(lambda b: tail_copy(k, b).start())

    def send_lates():
        lax.fori_loop(0, lates, send_late, None)
        lax.fori_loop(first_tail, chunks, send_own, None)

    def drain_y(k):
        y_copy(k).wait_send()

    def sent(k, count, semaphore):
        ref = merged.at[k, 0:count * rows]
        remote(ref, ref, semaphore, semaphore, y_peer).wait_send()

    def drain_z(k):
        sent(k, line - 1, z_send.at[k % ring])

    def drain_late(k):
        sent(k, 2 * (line - 1), zx_send.at[k // period % late_ring])

    lax.fori_loop(0, steps, step, 0)

    def all_late():
        return remote(late_y, late_y, late_send, late_recv, y_peer)

    def add_late(j, _):
        k = late_chunk(j)
        put(k, block(k, own, z)[...] + late_y[j])
        return 0

    all_late().wait_recv()
    lax.fori_loop(0, lates, add_late, 0)
    lax.fori_loop(first_tail, chunks, finish_tail, None)

    totals = counted[...]
    for d in range(1, experts):
        sender = lax.rem(e + d, experts)
        count_copy(d, sender).wait_recv()
        totals = totals + seen[sender]
    for layer in range(layers):
        share = jnp.sum(jnp.sum(squares[layer], axis=0, keepdims=True), axis=1, keepdims=True)
        totals = jnp.where(row == layer, share, totals)
    message[...] = totals
    gathered[me] = totals

    def all_copy(d, sender):
        return remote(
            message, gathered.at[sender], all_send, all_recv, group_peer(d)[1]
        )

    for d in range(1, group):
        all_copy(d, me).start()
    def drain_rest(k, _):
        drain_z(k)
        sent(k, line, tail_send.at[k - first_tail])

    for k in range(chunks - min(SLOTS, chunks), chunks):
        core_copy(k).wait_send()
    lax.fori_loop(
        steps - behind, first_tail, lambda k, _: when_chain(k, drain_z), None
    )
    lax.fori_loop(first_tail, chunks, drain_rest, None)
    all_late().wait_send()

    def all_others():
        others = gathered.at[0:group - 1]
        return remote(others, others, all_send, all_recv, y_peer)

    all_others().wait_recv()
    total = gathered[0]
    for p in range(1, group):
        total = total + gathered[p]
    stats = jnp.zeros_like(total)
    for layer in range(layers):
        loads = total[layers + layer:layers + layer + 1, :]
        spot = lane[:1]
        own_load = jnp.sum(jnp.where(spot == e, loads, 0.0), axis=1, keepdims=True)
        mean_load = jnp.sum(jnp.where(spot < experts, loads, 0.0), axis=1, keepdims=True) / experts
        root_mean = jnp.sqrt(total[layer:layer + 1, :1] / numel)
        factor = (
            step_size * (own_load / mean_load) * clip_level / jnp.maximum(root_mean, clip_level)
        )
        beta = own_load / (own_load + mean_load)
        stats = jnp.where(row == layer, factor, stats)
        stats = jnp.where(row == layers + layer, beta, stats)
    stat_ref[...] = stats

    all_others().wait_send()
    for d in range(1, experts):
        count_copy(d, e).wait_send()


def on_device(sizes, activations, out_grads, weights, shadow, counts):
    line, experts, shards = sizes
    layers, _, tokens, all_rows = activations.shape
    ff, rows = out_grads.shape[3], weights.shape[2]
    assert shards == 2 * CORES and 2 * layers <= 8
    units = ff // 128
    per_layer = next(
        p for p in range(PIECES, units + 1) if units % p == 0 and units // p % 2 == 0
    )
    width = ff // per_layer
    chunks = layers * per_layer
    half = line * rows
    group = line * shards
    period = max(2, 2 * (line - 1))
    lates = chunks // period - FEWER
    period = max(2, period - CUT)
    ring = HOP * (line - 1) + HOP + 3
    y_ring = 2 * LAG + 2
    assert (lates - 1) * period + 1 < chunks - TAIL
    late_ring = min(lates, -(-(HOP_LATE * (line - 1) + HOP + 6) // period))
    f32 = jnp.float32
    dma = pltpu.SemaphoreType.DMA
    vmem = pl.BlockSpec(memory_space=pltpu.VMEM)
    hbm = pl.BlockSpec(memory_space=pltpu.HBM)
    dims = (
        line, experts, shards, layers, per_layer, width, rows, all_rows * ff, period, lates, ring,
        late_ring, y_ring,
    )
    summed, stats = pl.pallas_call(
        functools.partial(kernel, dims),
        out_shape=(
            jax.ShapeDtypeStruct((layers, rows, ff), f32), jax.ShapeDtypeStruct((8, 128), f32)
        ),
        in_specs=[hbm] * 3,
        out_specs=(vmem, vmem),
        scratch_shapes=[
            pltpu.VMEM((layers, tokens, all_rows), activations.dtype),
            pltpu.SMEM((layers, 1, experts), jnp.int32),
            pltpu.VMEM((CORES, 2 * half, tokens), f32),
            pltpu.VMEM((layers, CORES, 2 * half, tokens), activations.dtype),
            pltpu.VMEM((RING, tokens, width), out_grads.dtype),
            pltpu.VMEM((chunks, 2 * half, width), f32),
            pltpu.VMEM((chunks, half, width), f32),
            pltpu.VMEM((chunks, line + 1, rows, width), f32),
            pltpu.VMEM((lates, 2 * (line + 1), rows, width), f32),
            pltpu.VMEM((lates, rows, width), f32),
            pltpu.VMEM((SLOTS, 2 * half, width), f32),
            pltpu.VMEM((layers, rows, width), f32),
            pltpu.VMEM((8, 128), f32),
            pltpu.VMEM((experts, 8, 128), f32),
            pltpu.VMEM((8, 128), f32),
            pltpu.VMEM((group, 8, 128), f32),
            dma, dma, dma((RING,)),
            dma((SLOTS,)), dma((SLOTS,)), dma((y_ring,)), dma((y_ring,)),
            dma((TAIL,)), dma((TAIL, line)),
            dma((ring,)), dma((ring, line + 1)),
            dma((late_ring,)), dma((late_ring, 2 * (line + 1))),
            dma, dma, dma((experts,)), dma((experts,)), dma, dma,
        ],
        compiler_params=pltpu.CompilerParams(
            collective_id=0, has_side_effects=True, vmem_limit_bytes=46 * 1024 * 1024
        ),
        name="reduce_gradient",
    )(
        pltpu.with_memory_space_constraint(activations[:, 0], pltpu.HBM), out_grads[:, 0],
        pltpu.with_memory_space_constraint(counts, pltpu.HBM),
    )
    factor = stats[:layers, 0][:, None, None]
    beta = stats[layers:2 * layers, 0][:, None, None]
    updated = weights[:, 0] - factor * summed
    previous = shadow[:, 0]
    return updated[:, None], (previous + beta * (updated - previous))[:, None]


def solution(mesh):
    rows = P(None, "expert", ("dp", "shard"), None)
    in_specs = (rows, rows, rows, rows, P(None, ("dp", "expert", "shard"), None))
    sizes = tuple(mesh.shape[a] for a in ("dp", "expert", "shard"))
    return jax.shard_map(
        functools.partial(on_device, sizes), mesh=mesh, in_specs=in_specs,
        out_specs=(rows, rows), check_vma=False,
    )
```

```python
import functools

import jax
import jax.numpy as jnp
from jax import lax
from jax.experimental import pallas as pl
from jax.experimental.pallas import tpu as pltpu
from jax.sharding import PartitionSpec as P

step_size = 0.5
clip_level = 1.0
CORES = 2
SLOTS = 4
LAG = 6
HOP = 3
HOP_LATE = 3
TAIL = 6
SPLIT = 4
AHEAD = 6
RING = 8
CUT = 0
FEWER = 0
PIECES = 28
MESH = pl.DeviceIdType.MESH


def kernel(
    dims, act_hbm, cot_hbm, cnt_hbm, out_ref, stat_ref,
    acts, cnt, turned, rows_ref, cot, merged, from_y, from_z, from_zx, late_y, staged,
    squares, counted, seen, message, gathered,
    act_sem, cnt_sem, cot_sem, core_send, core_recv, y_send, y_recv, tail_send, tail_recv, z_send, z_recv,
    zx_send, zx_recv, late_send, late_recv, cnt_send, cnt_recv, all_send, all_recv,
):
    line, experts, shards, layers, per_layer, width, rows, numel, period, lates, ring, late_ring, y_ring = dims
    group = line * shards
    half = line * rows
    chunks = layers * per_layer
    first_tail = chunks - TAIL
    z, e, s = lax.axis_index("dp"), lax.axis_index("expert"), lax.axis_index("shard")
    y, c = s // CORES, s % CORES
    me = z * shards + s
    core_peer = {"shard": y * CORES + (1 - c)}
    y_peer = {"shard": (1 - y) * CORES + c}
    own, other = y * half, (1 - y) * half

    def place(k):
        return k // per_layer, k % per_layer

    def columns(q):
        return pl.ds(pl.multiple_of(q * width, 128), width)

    def fetch(k):
        layer, q = place(k)
        return pltpu.make_async_copy(
            cot_hbm.at[layer, :, columns(q)], cot.at[k % RING], cot_sem.at[k % RING]
        )

    act_copy = pltpu.make_async_copy(act_hbm, acts, act_sem)
    cnt_fetch = pltpu.make_async_copy(cnt_hbm, cnt, cnt_sem)
    act_copy.start()
    fetch(0).start()

    def group_peer(d):
        p = lax.rem(me + d, group)
        return p, {"dp": p // shards, "shard": p % shards}

    def remote(src, dst, send, recv, device):
        return pltpu.make_async_remote_copy(
            src_ref=src, dst_ref=dst, send_sem=send, recv_sem=recv,
            device_id=device, device_id_type=MESH,
        )

    barrier = pltpu.get_barrier_semaphore()
    def greet(device):
        pl.semaphore_signal(barrier, inc=1, device_id=device, device_id_type=MESH)

    greet(core_peer)
    greet(y_peer)
    pl.when(z > 0)(lambda: greet({"dp": z - 1}))
    pl.when(z < line - 1)(lambda: greet({"dp": z + 1}))
    for d in range(1, experts):
        greet({"expert": lax.rem(e + d, experts)})
    for k in range(1, min(AHEAD, chunks)):
        fetch(k).start()
    cnt_fetch.start()

    def turn(layer):
        across = acts[layer].astype(jnp.float32).T
        for b in range(line):
            for h in range(shards // CORES):
                for core in range(CORES):
                    at = ((b * (shards // CORES) + h) * CORES + core) * rows
                    to = (h * line + b) * rows
                    turned[core, to:to + rows, :] = across[at:at + rows]
        for core in range(CORES):
            rows_ref[layer, core] = turned[core].astype(rows_ref.dtype)

    act_copy.wait()
    turn(0)
    ends = (z == 0).astype(jnp.int32) + (z == line - 1).astype(jnp.int32)
    pl.semaphore_wait(barrier, experts + 3 - ends)

    row = lax.broadcasted_iota(jnp.int32, counted.shape, 0)
    lane = lax.broadcasted_iota(jnp.int32, counted.shape, 1)

    def count_copy(d, sender):
        return remote(
            counted, seen.at[sender], cnt_send.at[d], cnt_recv.at[sender],
            {"expert": lax.rem(e + d, experts)},
        )

    def prepare():
        for layer in range(1, layers):
            turn(layer)
        cnt_fetch.wait()
        tile = jnp.zeros(counted.shape, jnp.float32)
        for layer in range(layers):
            for p in range(experts):
                here = (row == layers + layer) & (lane == p)
                tile = jnp.where(here, cnt[layer, 0, p].astype(jnp.float32), tile)
        counted[...] = tile
        squares[...] = jnp.zeros_like(squares)
        for d in range(1, experts):
            count_copy(d, e).start()

    def is_late(k):
        return (k % period == 1) & (k < period * lates)

    def late_chunk(j):
        return j * period + 1

    def when_chunk(k, body):
        pl.when((k >= 0) & (k < chunks))(lambda: body(k))

    def when_early(k, body):
        when_chunk(k, lambda k: pl.when(jnp.logical_not(is_late(k)))(lambda: body(k)))

    def when_chain(k, body):
        when_early(k, lambda k: pl.when(k < first_tail)(lambda: body(k)))

    def when_tail(k, body):
        pl.when((k >= first_tail) & (k < chunks))(lambda: body(k))

    def when_late(k, body):
        when_chunk(k, lambda k: pl.when(is_late(k))(lambda: body(k)))

    def core_copy(k):
        return remote(
            staged.at[k % SLOTS], merged.at[k], core_send.at[k % SLOTS], core_recv.at[k % SLOTS], core_peer
        )

    def y_copy(k):
        return remote(
            merged.at[k, pl.ds(pl.multiple_of(other, 8), half)], from_y.at[k],
            y_send.at[k % y_ring], y_recv.at[k % y_ring], y_peer,
        )

    def late_copy(k):
        j = k // period
        return remote(
            merged.at[k, pl.ds(pl.multiple_of(other + z * rows, 8), rows)], late_y.at[j],
            late_send, late_recv, y_peer,
        )

    def product(k, core):
        layer, _ = place(k)
        return jnp.dot(
            rows_ref[layer, core], cot[k % RING], preferred_element_type=jnp.float32
        )

    def stage_partner(k):
        pl.when(k >= SLOTS)(lambda: core_copy(k - SLOTS).wait_send())
        fetch(k).wait()
        staged[k % SLOTS] = product(k, 1 - c)
        core_copy(k).start()

    def merge_core(k):
        core_copy(k).wait_recv()
        merged[k] = merged[k] + product(k, c)
        when_chain(k, lambda k: y_copy(k).start())
        when_tail(k, lambda k: other_blocks(lambda b: tail_copy(k, b).start()))

    def tail_copy(k, b):
        i = k - first_tail
        at = pl.ds(pl.multiple_of(other + b * rows, 8), rows)
        return remote(
            merged.at[k, at], from_y.at[k, b * rows:(b + 1) * rows],
            tail_send.at[i], tail_recv.at[i, b], y_peer,
        )

    def other_blocks(body):
        for b in range(line):
            pl.when(z != b)(lambda: body(b))

    def own_block(body):
        for b in range(line):
            pl.when(z == b)(lambda: body(b))

    def merge_y(k):
        y_copy(k).wait_recv()
        at = pl.ds(pl.multiple_of(own, 8), half)
        merged[k, at, :] = merged[k, at, :] + from_y[k]

    def merge_block(k, b):
        tail_copy(k, b).wait_recv()
        at = pl.ds(pl.multiple_of(own + b * rows, 8), rows)
        merged[k, at, :] = merged[k, at, :] + from_y[k, b * rows:(b + 1) * rows, :]

    def merge_tail(k):
        other_blocks(lambda b: merge_block(k, b))

    def block(k, base, b):
        return merged.at[k, pl.ds(pl.multiple_of(base + b * rows, 8), rows)]

    def z_copy(k, base, b, slot, device, late):
        if late is None:
            return remote(
                block(k, base, b), from_z.at[k, slot], z_send.at[k % ring],
                z_recv.at[k % ring, slot], device,
            )
        j = k // period
        n = late * (line + 1) + slot
        return remote(
            block(k, base, b), from_zx.at[j, n], zx_send.at[j % late_ring],
            zx_recv.at[j % late_ring, n], device,
        )

    def arrived(k, slot, late):
        if late is None:
            return from_z[k, slot]
        return from_zx[k // period, late * (line + 1) + slot]

    def add_arrived(k, base, b, slot, late):
        z_copy(k, base, b, slot, {"dp": z}, late).wait_recv()
        ref = block(k, base, b)
        ref[...] = ref[...] + arrived(k, slot, late)

    def send_right(k, base, b, late):
        @pl.when(z < b)
        def _():
            pl.when(z > 0)(lambda: add_arrived(k, base, b, b + 1, late))
            z_copy(k, base, b, b + 1, {"dp": z + 1}, late).start()

    def send_left(k, base, b, late):
        @pl.when(z > b)
        def _():
            pl.when(z < line - 1)(lambda: add_arrived(k, base, b, b, late))
            z_copy(k, base, b, b, {"dp": z - 1}, late).start()

    def to_right(k, base, late):
        for b in reversed(range(1, line)):
            send_right(k, base, b, late)

    def to_left(k, base, late):
        for b in range(line - 1):
            send_left(k, base, b, late)

    def far_right(k):
        for b in reversed(range(2, line)):
            pl.when(z + 1 < b)(lambda: send_right(k, own, b, None))

    def far_left(k):
        for b in range(line - 2):
            pl.when(z - 1 > b)(lambda: send_left(k, own, b, None))

    def near_right(k, _):
        for b in range(1, line):
            pl.when(z + 1 == b)(lambda: send_right(k, own, b, None))

    def near_left(k, _):
        for b in range(line - 1):
            pl.when(z - 1 == b)(lambda: send_left(k, own, b, None))

    def both_halves(one):
        def body(k):
            one(k, other, 0)
            one(k, own, 1)
        return body

    def own_half(one):
        return lambda k: one(k, own, None)

    def put(k, values):
        layer, q = place(k)
        out_ref[layer, :, columns(q)] = values
        squares[layer] = squares[layer] + values * values

    def gather_block(k, base, late):
        pl.when(z > 0)(lambda: add_arrived(k, base, z, z + 1, late))
        pl.when(z < line - 1)(lambda: add_arrived(k, base, z, z, late))

    def finish_early(k):
        gather_block(k, own, None)
        put(k, block(k, own, z)[...])

    def finish_tail(k, _):
        own_block(lambda b: merge_block(k, b))
        finish_early(k)

    def finish_late(k):
        gather_block(k, other, 0)
        gather_block(k, own, 1)

    back = line - 1 - z
    far = jnp.maximum(z, back)

    def on_tail(body):
        return lambda: lax.fori_loop(first_tail, chunks, body, None)

    def step(t, _):
        pl.when(t + AHEAD < chunks)(lambda: fetch(t + AHEAD).start())
        when_chunk(t, stage_partner)
        when_chunk(t - 1, merge_core)
        when_late(t - 1 - HOP_LATE * z, both_halves(to_right))
        when_late(t - 1 - HOP_LATE * back, both_halves(to_left))
        when_late(t - 1 - HOP_LATE * far, finish_late)
        pl.when(t == 2)(prepare)
        when_chain(t - LAG, merge_y)
        when_tail(t - LAG, merge_tail)
        when_chain(t - LAG - HOP * z, own_half(to_right))
        when_chain(t - LAG - HOP * back, own_half(to_left))
        when_chain(t - LAG - HOP * far, finish_early)
        when_tail(t - LAG - HOP * z, far_right)
        when_tail(t - LAG - HOP * back, far_left)
        pl.when(t == chunks - 1 + LAG + HOP * z)(on_tail(near_right))
        pl.when(t == chunks - 1 + LAG + HOP * back)(on_tail(near_left))
        pl.when(t == start_late)(send_lates)
        when_chain(t - LAG - 1, drain_y)
        when_late(t - late_behind, drain_late)
        when_chain(t - behind, drain_z)
        return 0

    late_end = late_chunk(lates - 1) + 1 + HOP_LATE * (line - 1)
    start_late = max(chunks, late_end)
    behind = LAG + HOP * (line - 1) + 3
    late_behind = HOP_LATE * (line - 1) + 3
    steps = max(chunks + LAG + HOP * (line - 1), start_late + 1)

    def send_late(j, _):
        late_copy(late_chunk(j)).start()

    def send_own(k, _):
        own_block(lambda b: tail_copy(k, b).start())

    def send_lates():
        lax.fori_loop(0, lates, send_late, None)
        lax.fori_loop(first_tail, chunks, send_own, None)

    def drain_y(k):
        y_copy(k).wait_send()

    def sent(k, count, semaphore):
        ref = merged.at[k, 0:count * rows]
        remote(ref, ref, semaphore, semaphore, y_peer).wait_send()

    def drain_z(k):
        sent(k, line - 1, z_send.at[k % ring])

    def drain_late(k):
        sent(k, 2 * (line - 1), zx_send.at[k // period % late_ring])

    lax.fori_loop(0, steps, step, 0)

    def all_late():
        return remote(late_y, late_y, late_send, late_recv, y_peer)

    def add_late(j, _):
        k = late_chunk(j)
        put(k, block(k, own, z)[...] + late_y[j])
        return 0

    all_late().wait_recv()
    lax.fori_loop(0, lates, add_late, 0)
    lax.fori_loop(first_tail, chunks, finish_tail, None)

    totals = counted[...]
    for d in range(1, experts):
        sender = lax.rem(e + d, experts)
        count_copy(d, sender).wait_recv()
        totals = totals + seen[sender]
    for layer in range(layers):
        share = jnp.sum(jnp.sum(squares[layer], axis=0, keepdims=True), axis=1, keepdims=True)
        totals = jnp.where(row == layer, share, totals)
    message[...] = totals
    gathered[me] = totals

    def all_copy(d, sender):
        return remote(
            message, gathered.at[sender], all_send, all_recv, group_peer(d)[1]
        )

    for d in range(1, group):
        all_copy(d, me).start()
    def drain_rest(k, _):
        drain_z(k)
        sent(k, line, tail_send.at[k - first_tail])

    for k in range(chunks - min(SLOTS, chunks), chunks):
        core_copy(k).wait_send()
    lax.fori_loop(
        steps - behind, first_tail, lambda k, _: when_chain(k, drain_z), None
    )
    lax.fori_loop(first_tail, chunks, drain_rest, None)
    all_late().wait_send()

    def all_others():
        others = gathered.at[0:group - 1]
        return remote(others, others, all_send, all_recv, y_peer)

    all_others().wait_recv()
    total = gathered[0]
    for p in range(1, group):
        total = total + gathered[p]
    stats = jnp.zeros_like(total)
    for layer in range(layers):
        loads = total[layers + layer:layers + layer + 1, :]
        spot = lane[:1]
        own_load = jnp.sum(jnp.where(spot == e, loads, 0.0), axis=1, keepdims=True)
        mean_load = jnp.sum(jnp.where(spot < experts, loads, 0.0), axis=1, keepdims=True) / experts
        root_mean = jnp.sqrt(total[layer:layer + 1, :1] / numel)
        factor = (
            step_size * (own_load / mean_load) * clip_level / jnp.maximum(root_mean, clip_level)
        )
        beta = own_load / (own_load + mean_load)
        stats = jnp.where(row == layer, factor, stats)
        stats = jnp.where(row == layers + layer, beta, stats)
    stat_ref[...] = stats

    all_others().wait_send()
    for d in range(1, experts):
        count_copy(d, e).wait_send()


def update(
    layers, ff, stats, summed, weights, shadow, new_weights, new_shadow, updated, smoothed,
    weights_sem, shadow_sem,
):
    width = ff // SPLIT
    for layer in range(layers):
        factor = stats[layer:layer + 1, :1]
        beta = stats[layers + layer:layers + layer + 1, :1]
        for p in range(SPLIT):
            at = slice(p * width, (p + 1) * width)
            fresh = weights[layer, :, at] - factor * summed[layer, :, at]
            previous = shadow[layer, :, at]
            updated[layer, :, at] = fresh
            smoothed[layer, :, at] = previous + beta * (fresh - previous)
            pltpu.make_async_copy(
                updated.at[layer, :, at], new_weights.at[layer, :, at], weights_sem
            ).start()
            pltpu.make_async_copy(
                smoothed.at[layer, :, at], new_shadow.at[layer, :, at], shadow_sem
            ).start()
    pltpu.make_async_copy(updated, new_weights, weights_sem).wait()
    pltpu.make_async_copy(smoothed, new_shadow, shadow_sem).wait()


def on_device(sizes, activations, out_grads, weights, shadow, counts):
    line, experts, shards = sizes
    layers, _, tokens, all_rows = activations.shape
    ff, rows = out_grads.shape[3], weights.shape[2]
    assert shards == 2 * CORES and 2 * layers <= 8
    units = ff // 128
    per_layer = next(
        p for p in range(PIECES, units + 1) if units % p == 0 and units // p % 2 == 0
    )
    width = ff // per_layer
    chunks = layers * per_layer
    half = line * rows
    group = line * shards
    period = max(2, 2 * (line - 1))
    lates = chunks // period - FEWER
    period = max(2, period - CUT)
    ring = HOP * (line - 1) + HOP + 3
    y_ring = 2 * LAG + 2
    assert (lates - 1) * period + 1 < chunks - TAIL
    late_ring = min(lates, -(-(HOP_LATE * (line - 1) + HOP + 6) // period))
    f32 = jnp.float32
    dma = pltpu.SemaphoreType.DMA
    vmem = pl.BlockSpec(memory_space=pltpu.VMEM)
    hbm = pl.BlockSpec(memory_space=pltpu.HBM)
    dims = (
        line, experts, shards, layers, per_layer, width, rows, all_rows * ff, period, lates, ring,
        late_ring, y_ring,
    )
    summed, stats = pl.pallas_call(
        functools.partial(kernel, dims),
        out_shape=(
            jax.ShapeDtypeStruct((layers, rows, ff), f32), jax.ShapeDtypeStruct((8, 128), f32)
        ),
        in_specs=[hbm] * 3,
        out_specs=(vmem, vmem),
        scratch_shapes=[
            pltpu.VMEM((layers, tokens, all_rows), activations.dtype),
            pltpu.SMEM((layers, 1, experts), jnp.int32),
            pltpu.VMEM((CORES, 2 * half, tokens), f32),
            pltpu.VMEM((layers, CORES, 2 * half, tokens), activations.dtype),
            pltpu.VMEM((RING, tokens, width), out_grads.dtype),
            pltpu.VMEM((chunks, 2 * half, width), f32),
            pltpu.VMEM((chunks, half, width), f32),
            pltpu.VMEM((chunks, line + 1, rows, width), f32),
            pltpu.VMEM((lates, 2 * (line + 1), rows, width), f32),
            pltpu.VMEM((lates, rows, width), f32),
            pltpu.VMEM((SLOTS, 2 * half, width), f32),
            pltpu.VMEM((layers, rows, width), f32),
            pltpu.VMEM((8, 128), f32),
            pltpu.VMEM((experts, 8, 128), f32),
            pltpu.VMEM((8, 128), f32),
            pltpu.VMEM((group, 8, 128), f32),
            dma, dma, dma((RING,)),
            dma((SLOTS,)), dma((SLOTS,)), dma((y_ring,)), dma((y_ring,)),
            dma((TAIL,)), dma((TAIL, line)),
            dma((ring,)), dma((ring, line + 1)),
            dma((late_ring,)), dma((late_ring, 2 * (line + 1))),
            dma, dma, dma((experts,)), dma((experts,)), dma, dma,
        ],
        compiler_params=pltpu.CompilerParams(
            collective_id=0, has_side_effects=True, vmem_limit_bytes=46 * 1024 * 1024
        ),
        name="reduce_gradient",
    )(
        pltpu.with_memory_space_constraint(activations[:, 0], pltpu.HBM), out_grads[:, 0],
        pltpu.with_memory_space_constraint(counts, pltpu.HBM),
    )
    updated, smoothed = pl.pallas_call(
        functools.partial(update, layers, ff),
        out_shape=(jax.ShapeDtypeStruct((layers, rows, ff), f32),) * 2,
        in_specs=[vmem] * 4,
        out_specs=(hbm, hbm),
        scratch_shapes=[
            pltpu.VMEM((layers, rows, ff), f32), pltpu.VMEM((layers, rows, ff), f32), dma, dma
        ],
        compiler_params=pltpu.CompilerParams(vmem_limit_bytes=12 * 1024 * 1024),
        name="update",
    )(stats, summed, weights[:, 0], shadow[:, 0])
    return updated[:, None], smoothed[:, None]


def solution(mesh):
    rows = P(None, "expert", ("dp", "shard"), None)
    in_specs = (rows, rows, rows, rows, P(None, ("dp", "expert", "shard"), None))
    sizes = tuple(mesh.shape[a] for a in ("dp", "expert", "shard"))
    return jax.shard_map(
        functools.partial(on_device, sizes), mesh=mesh, in_specs=in_specs,
        out_specs=(rows, rows), check_vma=False,
    )
```

```python
import functools

import jax
import jax.numpy as jnp
from jax import lax
from jax.experimental import pallas as pl
from jax.experimental.pallas import tpu as pltpu
from jax.sharding import PartitionSpec as P

step_size = 0.5
clip_level = 1.0
CORES = 2
SLOTS = 4
LAG = 6
HOP = 3
HOP_LATE = 3
TAIL = 6
SPLIT = 4
AHEAD = 6
RING = 8
CUT = 0
FEWER = 0
PIECES = 28
MESH = pl.DeviceIdType.MESH


def kernel(
    dims, act_hbm, cot_hbm, cnt_hbm, out_ref, stat_ref,
    acts, cnt, turned, rows_ref, cot, merged, from_y, from_z, from_zx, late_y, staged,
    squares, counted, seen, message, gathered,
    act_sem, cnt_sem, cot_sem, core_send, core_recv, y_send, y_recv, tail_send, tail_recv, z_send, z_recv,
    zx_send, zx_recv, late_send, late_recv, cnt_send, cnt_recv, all_send, all_recv,
):
    line, experts, shards, layers, per_layer, width, rows, numel, period, lates, ring, late_ring, y_ring = dims
    group = line * shards
    half = line * rows
    chunks = layers * per_layer
    first_tail = chunks - TAIL
    z, e, s = lax.axis_index("dp"), lax.axis_index("expert"), lax.axis_index("shard")
    y, c = s // CORES, s % CORES
    me = z * shards + s
    core_peer = {"shard": y * CORES + (1 - c)}
    y_peer = {"shard": (1 - y) * CORES + c}
    own, other = y * half, (1 - y) * half

    def place(k):
        return k // per_layer, k % per_layer

    def columns(q):
        return pl.ds(pl.multiple_of(q * width, 128), width)

    def fetch(k):
        layer, q = place(k)
        return pltpu.make_async_copy(
            cot_hbm.at[layer, :, columns(q)], cot.at[k % RING], cot_sem.at[k % RING]
        )

    act_copy = pltpu.make_async_copy(act_hbm, acts, act_sem)
    cnt_fetch = pltpu.make_async_copy(cnt_hbm, cnt, cnt_sem)
    act_copy.start()
    fetch(0).start()

    def group_peer(d):
        p = lax.rem(me + d, group)
        return p, {"dp": p // shards, "shard": p % shards}

    def remote(src, dst, send, recv, device):
        return pltpu.make_async_remote_copy(
            src_ref=src, dst_ref=dst, send_sem=send, recv_sem=recv,
            device_id=device, device_id_type=MESH,
        )

    barrier = pltpu.get_barrier_semaphore()
    def greet(device):
        pl.semaphore_signal(barrier, inc=1, device_id=device, device_id_type=MESH)

    greet(core_peer)
    greet(y_peer)
    pl.when(z > 0)(lambda: greet({"dp": z - 1}))
    pl.when(z < line - 1)(lambda: greet({"dp": z + 1}))
    for d in range(1, experts):
        greet({"expert": lax.rem(e + d, experts)})
    for k in range(1, min(AHEAD, chunks)):
        fetch(k).start()
    cnt_fetch.start()

    def turn(layer):
        across = acts[layer].astype(jnp.float32).T
        for b in range(line):
            for h in range(shards // CORES):
                for core in range(CORES):
                    at = ((b * (shards // CORES) + h) * CORES + core) * rows
                    to = (h * line + b) * rows
                    turned[core, to:to + rows, :] = across[at:at + rows]
        for core in range(CORES):
            rows_ref[layer, core] = turned[core].astype(rows_ref.dtype)

    act_copy.wait()
    turn(0)
    ends = (z == 0).astype(jnp.int32) + (z == line - 1).astype(jnp.int32)
    pl.semaphore_wait(barrier, experts + 3 - ends)

    row = lax.broadcasted_iota(jnp.int32, counted.shape, 0)
    lane = lax.broadcasted_iota(jnp.int32, counted.shape, 1)

    def count_copy(d, sender):
        return remote(
            counted, seen.at[sender], cnt_send.at[d], cnt_recv.at[sender],
            {"expert": lax.rem(e + d, experts)},
        )

    def prepare():
        for layer in range(1, layers):
            turn(layer)
        cnt_fetch.wait()
        tile = jnp.zeros(counted.shape, jnp.float32)
        for layer in range(layers):
            for p in range(experts):
                here = (row == layers + layer) & (lane == p)
                tile = jnp.where(here, cnt[layer, 0, p].astype(jnp.float32), tile)
        counted[...] = tile
        squares[...] = jnp.zeros_like(squares)
        for d in range(1, experts):
            count_copy(d, e).start()

    def is_late(k):
        return (k % period == 1) & (k < period * lates)

    def late_chunk(j):
        return j * period + 1

    def when_chunk(k, body):
        pl.when((k >= 0) & (k < chunks))(lambda: body(k))

    def when_early(k, body):
        when_chunk(k, lambda k: pl.when(jnp.logical_not(is_late(k)))(lambda: body(k)))

    def when_chain(k, body):
        when_early(k, lambda k: pl.when(k < first_tail)(lambda: body(k)))

    def when_tail(k, body):
        pl.when((k >= first_tail) & (k < chunks))(lambda: body(k))

    def when_late(k, body):
        when_chunk(k, lambda k: pl.when(is_late(k))(lambda: body(k)))

    def core_copy(k):
        return remote(
            staged.at[k % SLOTS], merged.at[k], core_send.at[k % SLOTS], core_recv.at[k % SLOTS], core_peer
        )

    def y_copy(k):
        return remote(
            merged.at[k, pl.ds(pl.multiple_of(other, 8), half)], from_y.at[k],
            y_send.at[k % y_ring], y_recv.at[k % y_ring], y_peer,
        )

    def late_copy(k):
        j = k // period
        return remote(
            merged.at[k, pl.ds(pl.multiple_of(other + z * rows, 8), rows)], late_y.at[j],
            late_send, late_recv, y_peer,
        )

    def product(k, core):
        layer, _ = place(k)
        return jnp.dot(
            rows_ref[layer, core], cot[k % RING], preferred_element_type=jnp.float32
        )

    def stage_partner(k):
        pl.when(k >= SLOTS)(lambda: core_copy(k - SLOTS).wait_send())
        fetch(k).wait()
        staged[k % SLOTS] = product(k, 1 - c)
        core_copy(k).start()

    def merge_core(k):
        core_copy(k).wait_recv()
        merged[k] = merged[k] + product(k, c)
        when_chain(k, lambda k: y_copy(k).start())
        when_tail(k, lambda k: other_blocks(lambda b: tail_copy(k, b).start()))

    def tail_copy(k, b):
        i = k - first_tail
        at = pl.ds(pl.multiple_of(other + b * rows, 8), rows)
        return remote(
            merged.at[k, at], from_y.at[k, b * rows:(b + 1) * rows],
            tail_send.at[i], tail_recv.at[i, b], y_peer,
        )

    def other_blocks(body):
        for b in range(line):
            pl.when(z != b)(lambda: body(b))

    def own_block(body):
        for b in range(line):
            pl.when(z == b)(lambda: body(b))

    def merge_y(k):
        y_copy(k).wait_recv()
        at = pl.ds(pl.multiple_of(own, 8), half)
        merged[k, at, :] = merged[k, at, :] + from_y[k]

    def merge_block(k, b):
        tail_copy(k, b).wait_recv()
        at = pl.ds(pl.multiple_of(own + b * rows, 8), rows)
        merged[k, at, :] = merged[k, at, :] + from_y[k, b * rows:(b + 1) * rows, :]

    def merge_tail(k):
        other_blocks(lambda b: merge_block(k, b))

    def block(k, base, b):
        return merged.at[k, pl.ds(pl.multiple_of(base + b * rows, 8), rows)]

    def z_copy(k, base, b, slot, device, late):
        if late is None:
            return remote(
                block(k, base, b), from_z.at[k, slot], z_send.at[k % ring],
                z_recv.at[k % ring, slot], device,
            )
        j = k // period
        n = late * (line + 1) + slot
        return remote(
            block(k, base, b), from_zx.at[j, n], zx_send.at[j % late_ring],
            zx_recv.at[j % late_ring, n], device,
        )

    def arrived(k, slot, late):
        if late is None:
            return from_z[k, slot]
        return from_zx[k // period, late * (line + 1) + slot]

    def add_arrived(k, base, b, slot, late):
        z_copy(k, base, b, slot, {"dp": z}, late).wait_recv()
        ref = block(k, base, b)
        ref[...] = ref[...] + arrived(k, slot, late)

    def send_right(k, base, b, late):
        @pl.when(z < b)
        def _():
            pl.when(z > 0)(lambda: add_arrived(k, base, b, b + 1, late))
            z_copy(k, base, b, b + 1, {"dp": z + 1}, late).start()

    def send_left(k, base, b, late):
        @pl.when(z > b)
        def _():
            pl.when(z < line - 1)(lambda: add_arrived(k, base, b, b, late))
            z_copy(k, base, b, b, {"dp": z - 1}, late).start()

    def to_right(k, base, late):
        for b in reversed(range(1, line)):
            send_right(k, base, b, late)

    def to_left(k, base, late):
        for b in range(line - 1):
            send_left(k, base, b, late)

    def far_right(k):
        for b in reversed(range(2, line)):
            send_right(k, own, b, None)

    def far_left(k):
        for b in range(line - 2):
            send_left(k, own, b, None)

    def near_right(k, _):
        send_right(k, own, 1, None)

    def near_left(k, _):
        send_left(k, own, line - 2, None)

    def both_halves(one):
        def body(k):
            one(k, other, 0)
            one(k, own, 1)
        return body

    def own_half(one):
        return lambda k: one(k, own, None)

    def put(k, values):
        layer, q = place(k)
        out_ref[layer, :, columns(q)] = values
        squares[layer] = squares[layer] + values * values

    def gather_block(k, base, late):
        pl.when(z > 0)(lambda: add_arrived(k, base, z, z + 1, late))
        pl.when(z < line - 1)(lambda: add_arrived(k, base, z, z, late))

    def finish_early(k):
        gather_block(k, own, None)
        put(k, block(k, own, z)[...])

    def finish_tail(k, _):
        own_block(lambda b: merge_block(k, b))
        finish_early(k)

    def finish_late(k):
        gather_block(k, other, 0)
        gather_block(k, own, 1)

    back = line - 1 - z
    far = jnp.maximum(z, back)

    def on_tail(body):
        return lambda: lax.fori_loop(first_tail, chunks, body, None)

    def step(t, _):
        pl.when(t + AHEAD < chunks)(lambda: fetch(t + AHEAD).start())
        when_chunk(t, stage_partner)
        when_chunk(t - 1, merge_core)
        when_late(t - 1 - HOP_LATE * z, both_halves(to_right))
        when_late(t - 1 - HOP_LATE * back, both_halves(to_left))
        when_late(t - 1 - HOP_LATE * far, finish_late)
        pl.when(t == 2)(prepare)
        when_chain(t - LAG, merge_y)
        when_tail(t - LAG, merge_tail)
        when_chain(t - LAG - HOP * z, own_half(to_right))
        when_chain(t - LAG - HOP * back, own_half(to_left))
        when_chain(t - LAG - HOP * far, finish_early)
        when_tail(t - LAG - HOP * z, far_right)
        when_tail(t - LAG - HOP * back, far_left)
        pl.when((t == chunks - 1 + LAG) & (z == 0))(on_tail(near_right))
        pl.when((t == chunks - 1 + LAG) & (back == 0))(on_tail(near_left))
        pl.when(t == start_late)(send_lates)
        when_chain(t - LAG - 1, drain_y)
        when_late(t - late_behind, drain_late)
        when_chain(t - behind, drain_z)
        return 0

    late_end = late_chunk(lates - 1) + 1 + HOP_LATE * (line - 1)
    start_late = max(chunks, late_end)
    behind = LAG + HOP * (line - 1) + 3
    late_behind = HOP_LATE * (line - 1) + 3
    steps = max(chunks + LAG + HOP * (line - 1), start_late + 1)

    def send_late(j, _):
        late_copy(late_chunk(j)).start()

    def send_own(k, _):
        own_block(lambda b: tail_copy(k, b).start())

    def send_lates():
        lax.fori_loop(0, lates, send_late, None)
        lax.fori_loop(first_tail, chunks, send_own, None)

    def drain_y(k):
        y_copy(k).wait_send()

    def sent(k, count, semaphore):
        ref = merged.at[k, 0:count * rows]
        remote(ref, ref, semaphore, semaphore, y_peer).wait_send()

    def drain_z(k):
        sent(k, line - 1, z_send.at[k % ring])

    def drain_late(k):
        sent(k, 2 * (line - 1), zx_send.at[k // period % late_ring])

    lax.fori_loop(0, steps, step, 0)

    def all_late():
        return remote(late_y, late_y, late_send, late_recv, y_peer)

    def add_late(j, _):
        k = late_chunk(j)
        put(k, block(k, own, z)[...] + late_y[j])
        return 0

    all_late().wait_recv()
    lax.fori_loop(0, lates, add_late, 0)
    lax.fori_loop(first_tail, chunks, finish_tail, None)

    totals = counted[...]
    for d in range(1, experts):
        sender = lax.rem(e + d, experts)
        count_copy(d, sender).wait_recv()
        totals = totals + seen[sender]
    for layer in range(layers):
        share = jnp.sum(jnp.sum(squares[layer], axis=0, keepdims=True), axis=1, keepdims=True)
        totals = jnp.where(row == layer, share, totals)
    message[...] = totals
    gathered[me] = totals

    def all_copy(d, sender):
        return remote(
            message, gathered.at[sender], all_send, all_recv, group_peer(d)[1]
        )

    for d in range(1, group):
        all_copy(d, me).start()
    def drain_rest(k, _):
        drain_z(k)
        sent(k, line, tail_send.at[k - first_tail])

    for k in range(chunks - min(SLOTS, chunks), chunks):
        core_copy(k).wait_send()
    lax.fori_loop(
        steps - behind, first_tail, lambda k, _: when_chain(k, drain_z), None
    )
    lax.fori_loop(first_tail, chunks, drain_rest, None)
    all_late().wait_send()

    def all_others():
        others = gathered.at[0:group - 1]
        return remote(others, others, all_send, all_recv, y_peer)

    all_others().wait_recv()
    total = gathered[0]
    for p in range(1, group):
        total = total + gathered[p]
    stats = jnp.zeros_like(total)
    for layer in range(layers):
        loads = total[layers + layer:layers + layer + 1, :]
        spot = lane[:1]
        own_load = jnp.sum(jnp.where(spot == e, loads, 0.0), axis=1, keepdims=True)
        mean_load = jnp.sum(jnp.where(spot < experts, loads, 0.0), axis=1, keepdims=True) / experts
        root_mean = jnp.sqrt(total[layer:layer + 1, :1] / numel)
        factor = (
            step_size * (own_load / mean_load) * clip_level / jnp.maximum(root_mean, clip_level)
        )
        beta = own_load / (own_load + mean_load)
        stats = jnp.where(row == layer, factor, stats)
        stats = jnp.where(row == layers + layer, beta, stats)
    stat_ref[...] = stats

    all_others().wait_send()
    for d in range(1, experts):
        count_copy(d, e).wait_send()


def update(
    layers, ff, stats, summed, weights, shadow, new_weights, new_shadow, updated, smoothed,
    weights_sem, shadow_sem,
):
    width = ff // SPLIT
    for layer in range(layers):
        factor = stats[layer:layer + 1, :1]
        beta = stats[layers + layer:layers + layer + 1, :1]
        for p in range(SPLIT):
            at = slice(p * width, (p + 1) * width)
            fresh = weights[layer, :, at] - factor * summed[layer, :, at]
            previous = shadow[layer, :, at]
            updated[layer, :, at] = fresh
            smoothed[layer, :, at] = previous + beta * (fresh - previous)
            pltpu.make_async_copy(
                updated.at[layer, :, at], new_weights.at[layer, :, at], weights_sem
            ).start()
            pltpu.make_async_copy(
                smoothed.at[layer, :, at], new_shadow.at[layer, :, at], shadow_sem
            ).start()
    pltpu.make_async_copy(updated, new_weights, weights_sem).wait()
    pltpu.make_async_copy(smoothed, new_shadow, shadow_sem).wait()


def on_device(sizes, activations, out_grads, weights, shadow, counts):
    line, experts, shards = sizes
    layers, _, tokens, all_rows = activations.shape
    ff, rows = out_grads.shape[3], weights.shape[2]
    assert shards == 2 * CORES and 2 * layers <= 8
    units = ff // 128
    per_layer = next(
        p for p in range(PIECES, units + 1) if units % p == 0 and units // p % 2 == 0
    )
    width = ff // per_layer
    chunks = layers * per_layer
    half = line * rows
    group = line * shards
    period = max(2, 2 * (line - 1))
    lates = chunks // period - FEWER
    period = max(2, period - CUT)
    ring = HOP * (line - 1) + HOP + 3
    y_ring = 2 * LAG + 2
    assert (lates - 1) * period + 1 < chunks - TAIL
    late_ring = min(lates, -(-(HOP_LATE * (line - 1) + HOP + 6) // period))
    f32 = jnp.float32
    dma = pltpu.SemaphoreType.DMA
    vmem = pl.BlockSpec(memory_space=pltpu.VMEM)
    hbm = pl.BlockSpec(memory_space=pltpu.HBM)
    dims = (
        line, experts, shards, layers, per_layer, width, rows, all_rows * ff, period, lates, ring,
        late_ring, y_ring,
    )
    summed, stats = pl.pallas_call(
        functools.partial(kernel, dims),
        out_shape=(
            jax.ShapeDtypeStruct((layers, rows, ff), f32), jax.ShapeDtypeStruct((8, 128), f32)
        ),
        in_specs=[hbm] * 3,
        out_specs=(vmem, vmem),
        scratch_shapes=[
            pltpu.VMEM((layers, tokens, all_rows), activations.dtype),
            pltpu.SMEM((layers, 1, experts), jnp.int32),
            pltpu.VMEM((CORES, 2 * half, tokens), f32),
            pltpu.VMEM((layers, CORES, 2 * half, tokens), activations.dtype),
            pltpu.VMEM((RING, tokens, width), out_grads.dtype),
            pltpu.VMEM((chunks, 2 * half, width), f32),
            pltpu.VMEM((chunks, half, width), f32),
            pltpu.VMEM((chunks, line + 1, rows, width), f32),
            pltpu.VMEM((lates, 2 * (line + 1), rows, width), f32),
            pltpu.VMEM((lates, rows, width), f32),
            pltpu.VMEM((SLOTS, 2 * half, width), f32),
            pltpu.VMEM((layers, rows, width), f32),
            pltpu.VMEM((8, 128), f32),
            pltpu.VMEM((experts, 8, 128), f32),
            pltpu.VMEM((8, 128), f32),
            pltpu.VMEM((group, 8, 128), f32),
            dma, dma, dma((RING,)),
            dma((SLOTS,)), dma((SLOTS,)), dma((y_ring,)), dma((y_ring,)),
            dma((TAIL,)), dma((TAIL, line)),
            dma((ring,)), dma((ring, line + 1)),
            dma((late_ring,)), dma((late_ring, 2 * (line + 1))),
            dma, dma, dma((experts,)), dma((experts,)), dma, dma,
        ],
        compiler_params=pltpu.CompilerParams(
            collective_id=0, has_side_effects=True, vmem_limit_bytes=46 * 1024 * 1024
        ),
        name="reduce_gradient",
    )(
        pltpu.with_memory_space_constraint(activations[:, 0], pltpu.HBM), out_grads[:, 0],
        pltpu.with_memory_space_constraint(counts, pltpu.HBM),
    )
    updated, smoothed = pl.pallas_call(
        functools.partial(update, layers, ff),
        out_shape=(jax.ShapeDtypeStruct((layers, rows, ff), f32),) * 2,
        in_specs=[vmem] * 4,
        out_specs=(hbm, hbm),
        scratch_shapes=[
            pltpu.VMEM((layers, rows, ff), f32), pltpu.VMEM((layers, rows, ff), f32), dma, dma
        ],
        compiler_params=pltpu.CompilerParams(vmem_limit_bytes=12 * 1024 * 1024),
        name="update",
    )(stats, summed, weights[:, 0], shadow[:, 0])
    return updated[:, None], smoothed[:, None]


def solution(mesh):
    rows = P(None, "expert", ("dp", "shard"), None)
    in_specs = (rows, rows, rows, rows, P(None, ("dp", "expert", "shard"), None))
    sizes = tuple(mesh.shape[a] for a in ("dp", "expert", "shard"))
    return jax.shard_map(
        functools.partial(on_device, sizes), mesh=mesh, in_specs=in_specs,
        out_specs=(rows, rows), check_vma=False,
    )
```

```python
import functools

import jax
import jax.numpy as jnp
from jax import lax
from jax.experimental import pallas as pl
from jax.experimental.pallas import tpu as pltpu
from jax.sharding import PartitionSpec as P

step_size = 0.5
clip_level = 1.0
CORES = 2
SLOTS = 4
LAG = 6
HOP = 3
HOP_LATE = 3
TAIL = 5
MID = 4
SPLIT = 4
AHEAD = 6
RING = 8
CUT = 0
FEWER = 0
PIECES = 28
MESH = pl.DeviceIdType.MESH


def kernel(
    dims, act_hbm, cot_hbm, cnt_hbm, out_ref, stat_ref,
    acts, cnt, turned, rows_ref, cot, merged, from_y, from_z, from_zx, late_y, staged,
    squares, counted, seen, message, gathered,
    act_sem, cnt_sem, cot_sem, core_send, core_recv, y_send, y_recv, tail_send, tail_recv, z_send, z_recv,
    zx_send, zx_recv, late_send, late_recv, cnt_send, cnt_recv, all_send, all_recv,
):
    line, experts, shards, layers, per_layer, width, rows, numel, period, lates, ring, late_ring, y_ring = dims
    group = line * shards
    half = line * rows
    chunks = layers * per_layer
    first_tail = chunks - TAIL
    first_mid = chunks - (MID if line > 3 else 0)
    z, e, s = lax.axis_index("dp"), lax.axis_index("expert"), lax.axis_index("shard")
    y, c = s // CORES, s % CORES
    me = z * shards + s
    core_peer = {"shard": y * CORES + (1 - c)}
    y_peer = {"shard": (1 - y) * CORES + c}
    own, other = y * half, (1 - y) * half

    def place(k):
        return k // per_layer, k % per_layer

    def columns(q):
        return pl.ds(pl.multiple_of(q * width, 128), width)

    def fetch(k):
        layer, q = place(k)
        return pltpu.make_async_copy(
            cot_hbm.at[layer, :, columns(q)], cot.at[k % RING], cot_sem.at[k % RING]
        )

    act_copy = pltpu.make_async_copy(act_hbm, acts, act_sem)
    cnt_fetch = pltpu.make_async_copy(cnt_hbm, cnt, cnt_sem)
    act_copy.start()
    fetch(0).start()

    def group_peer(d):
        p = lax.rem(me + d, group)
        return p, {"dp": p // shards, "shard": p % shards}

    def remote(src, dst, send, recv, device):
        return pltpu.make_async_remote_copy(
            src_ref=src, dst_ref=dst, send_sem=send, recv_sem=recv,
            device_id=device, device_id_type=MESH,
        )

    barrier = pltpu.get_barrier_semaphore()
    def greet(device):
        pl.semaphore_signal(barrier, inc=1, device_id=device, device_id_type=MESH)

    greet(core_peer)
    greet(y_peer)
    pl.when(z > 0)(lambda: greet({"dp": z - 1}))
    pl.when(z < line - 1)(lambda: greet({"dp": z + 1}))
    for d in range(1, experts):
        greet({"expert": lax.rem(e + d, experts)})
    for k in range(1, min(AHEAD, chunks)):
        fetch(k).start()
    cnt_fetch.start()

    def turn(layer):
        across = acts[layer].astype(jnp.float32).T
        for b in range(line):
            for h in range(shards // CORES):
                for core in range(CORES):
                    at = ((b * (shards // CORES) + h) * CORES + core) * rows
                    to = (h * line + b) * rows
                    turned[core, to:to + rows, :] = across[at:at + rows]
        for core in range(CORES):
            rows_ref[layer, core] = turned[core].astype(rows_ref.dtype)

    act_copy.wait()
    turn(0)
    ends = (z == 0).astype(jnp.int32) + (z == line - 1).astype(jnp.int32)
    pl.semaphore_wait(barrier, experts + 3 - ends)

    row = lax.broadcasted_iota(jnp.int32, counted.shape, 0)
    lane = lax.broadcasted_iota(jnp.int32, counted.shape, 1)

    def count_copy(d, sender):
        return remote(
            counted, seen.at[sender], cnt_send.at[d], cnt_recv.at[sender],
            {"expert": lax.rem(e + d, experts)},
        )

    def prepare():
        for layer in range(1, layers):
            turn(layer)
        cnt_fetch.wait()
        tile = jnp.zeros(counted.shape, jnp.float32)
        for layer in range(layers):
            for p in range(experts):
                here = (row == layers + layer) & (lane == p)
                tile = jnp.where(here, cnt[layer, 0, p].astype(jnp.float32), tile)
        counted[...] = tile
        squares[...] = jnp.zeros_like(squares)
        for d in range(1, experts):
            count_copy(d, e).start()

    def is_late(k):
        return (k % period == 1) & (k < period * lates)

    def late_chunk(j):
        return j * period + 1

    def when_chunk(k, body):
        pl.when((k >= 0) & (k < chunks))(lambda: body(k))

    def when_early(k, body):
        when_chunk(k, lambda k: pl.when(jnp.logical_not(is_late(k)))(lambda: body(k)))

    def when_chain(k, body):
        when_early(k, lambda k: pl.when(k < first_tail)(lambda: body(k)))

    def when_tail(k, body):
        pl.when((k >= first_tail) & (k < chunks))(lambda: body(k))

    def when_late(k, body):
        when_chunk(k, lambda k: pl.when(is_late(k))(lambda: body(k)))

    def core_copy(k):
        return remote(
            staged.at[k % SLOTS], merged.at[k], core_send.at[k % SLOTS], core_recv.at[k % SLOTS], core_peer
        )

    def y_copy(k):
        return remote(
            merged.at[k, pl.ds(pl.multiple_of(other, 8), half)], from_y.at[k],
            y_send.at[k % y_ring], y_recv.at[k % y_ring], y_peer,
        )

    def late_copy(k):
        j = k // period
        return remote(
            merged.at[k, pl.ds(pl.multiple_of(other + z * rows, 8), rows)], late_y.at[j],
            late_send, late_recv, y_peer,
        )

    def product(k, core):
        layer, _ = place(k)
        return jnp.dot(
            rows_ref[layer, core], cot[k % RING], preferred_element_type=jnp.float32
        )

    def stage_partner(k):
        pl.when(k >= SLOTS)(lambda: core_copy(k - SLOTS).wait_send())
        fetch(k).wait()
        staged[k % SLOTS] = product(k, 1 - c)
        core_copy(k).start()

    def merge_core(k):
        core_copy(k).wait_recv()
        merged[k] = merged[k] + product(k, c)
        when_chain(k, lambda k: y_copy(k).start())
        when_tail(k, lambda k: other_blocks(lambda b: tail_copy(k, b).start()))

    def tail_copy(k, b):
        i = k - first_tail
        at = pl.ds(pl.multiple_of(other + b * rows, 8), rows)
        return remote(
            merged.at[k, at], from_y.at[k, b * rows:(b + 1) * rows],
            tail_send.at[i], tail_recv.at[i, b], y_peer,
        )

    def other_blocks(body):
        for b in range(line):
            pl.when(z != b)(lambda: body(b))

    def own_block(body):
        for b in range(line):
            pl.when(z == b)(lambda: body(b))

    def merge_y(k):
        y_copy(k).wait_recv()
        at = pl.ds(pl.multiple_of(own, 8), half)
        merged[k, at, :] = merged[k, at, :] + from_y[k]

    def merge_block(k, b):
        tail_copy(k, b).wait_recv()
        at = pl.ds(pl.multiple_of(own + b * rows, 8), rows)
        merged[k, at, :] = merged[k, at, :] + from_y[k, b * rows:(b + 1) * rows, :]

    def merge_tail(k):
        other_blocks(lambda b: merge_block(k, b))

    def block(k, base, b):
        return merged.at[k, pl.ds(pl.multiple_of(base + b * rows, 8), rows)]

    def z_copy(k, base, b, slot, device, late):
        if late is None:
            return remote(
                block(k, base, b), from_z.at[k, slot], z_send.at[k % ring],
                z_recv.at[k % ring, slot], device,
            )
        j = k // period
        n = late * (line + 1) + slot
        return remote(
            block(k, base, b), from_zx.at[j, n], zx_send.at[j % late_ring],
            zx_recv.at[j % late_ring, n], device,
        )

    def arrived(k, slot, late):
        if late is None:
            return from_z[k, slot]
        return from_zx[k // period, late * (line + 1) + slot]

    def add_arrived(k, base, b, slot, late):
        z_copy(k, base, b, slot, {"dp": z}, late).wait_recv()
        ref = block(k, base, b)
        ref[...] = ref[...] + arrived(k, slot, late)

    def send_right(k, base, b, late):
        @pl.when(z < b)
        def _():
            pl.when(z > 0)(lambda: add_arrived(k, base, b, b + 1, late))
            z_copy(k, base, b, b + 1, {"dp": z + 1}, late).start()

    def send_left(k, base, b, late):
        @pl.when(z > b)
        def _():
            pl.when(z < line - 1)(lambda: add_arrived(k, base, b, b, late))
            z_copy(k, base, b, b, {"dp": z - 1}, late).start()

    def to_right(k, base, late):
        for b in reversed(range(1, line)):
            send_right(k, base, b, late)

    def to_left(k, base, late):
        for b in range(line - 1):
            send_left(k, base, b, late)

    def sooner(k, b, last):
        return k < first_mid if b == last and line > 3 else k >= 0

    def far_right(k):
        for b in reversed(range(2, line)):
            pl.when(sooner(k, b, 2))(lambda: send_right(k, own, b, None))

    def far_left(k):
        for b in range(line - 2):
            pl.when(sooner(k, b, line - 3))(lambda: send_left(k, own, b, None))

    def mid_right(k, _):
        send_right(k, own, 2, None)

    def mid_left(k, _):
        send_left(k, own, line - 3, None)

    def near_right(k, _):
        send_right(k, own, 1, None)

    def near_left(k, _):
        send_left(k, own, line - 2, None)

    def both_halves(one):
        def body(k):
            one(k, other, 0)
            one(k, own, 1)
        return body

    def own_half(one):
        return lambda k: one(k, own, None)

    def put(k, values):
        layer, q = place(k)
        out_ref[layer, :, columns(q)] = values
        squares[layer] = squares[layer] + values * values

    def gather_block(k, base, late):
        pl.when(z > 0)(lambda: add_arrived(k, base, z, z + 1, late))
        pl.when(z < line - 1)(lambda: add_arrived(k, base, z, z, late))

    def finish_early(k):
        gather_block(k, own, None)
        put(k, block(k, own, z)[...])

    def finish_tail(k, _):
        own_block(lambda b: merge_block(k, b))
        finish_early(k)

    def finish_late(k):
        gather_block(k, other, 0)
        gather_block(k, own, 1)

    back = line - 1 - z
    far = jnp.maximum(z, back)

    def on_tail(body):
        return lambda: lax.fori_loop(first_tail, chunks, body, None)

    def on_mid(body):
        return lambda: lax.fori_loop(first_mid, chunks, body, None)

    def step(t, _):
        pl.when(t + AHEAD < chunks)(lambda: fetch(t + AHEAD).start())
        when_chunk(t, stage_partner)
        when_chunk(t - 1, merge_core)
        when_late(t - 1 - HOP_LATE * z, both_halves(to_right))
        when_late(t - 1 - HOP_LATE * back, both_halves(to_left))
        when_late(t - 1 - HOP_LATE * far, finish_late)
        pl.when(t == 2)(prepare)
        when_chain(t - LAG, merge_y)
        when_tail(t - LAG, merge_tail)
        when_chain(t - LAG - HOP * z, own_half(to_right))
        when_chain(t - LAG - HOP * back, own_half(to_left))
        when_chain(t - LAG - HOP * far, finish_early)
        when_tail(t - LAG - HOP * z, far_right)
        when_tail(t - LAG - HOP * back, far_left)
        pl.when(t == chunks - 1 + LAG + HOP * z)(on_mid(mid_right))
        pl.when(t == chunks - 1 + LAG + HOP * back)(on_mid(mid_left))
        pl.when((t == chunks - 1 + LAG) & (z == 0))(on_tail(near_right))
        pl.when((t == chunks - 1 + LAG) & (back == 0))(on_tail(near_left))
        pl.when(t == start_late)(send_lates)
        when_chain(t - LAG - 1, drain_y)
        when_late(t - late_behind, drain_late)
        when_chain(t - behind, drain_z)
        return 0

    late_end = late_chunk(lates - 1) + 1 + HOP_LATE * (line - 1)
    start_late = max(chunks, late_end)
    behind = LAG + HOP * (line - 1) + 3
    late_behind = HOP_LATE * (line - 1) + 3
    steps = max(chunks + LAG + HOP * (line - 1), start_late + 1)

    def send_late(j, _):
        late_copy(late_chunk(j)).start()

    def send_own(k, _):
        own_block(lambda b: tail_copy(k, b).start())

    def send_lates():
        lax.fori_loop(0, lates, send_late, None)
        lax.fori_loop(first_tail, chunks, send_own, None)

    def drain_y(k):
        y_copy(k).wait_send()

    def sent(k, count, semaphore):
        ref = merged.at[k, 0:count * rows]
        remote(ref, ref, semaphore, semaphore, y_peer).wait_send()

    def drain_z(k):
        sent(k, line - 1, z_send.at[k % ring])

    def drain_late(k):
        sent(k, 2 * (line - 1), zx_send.at[k // period % late_ring])

    lax.fori_loop(0, steps, step, 0)

    def all_late():
        return remote(late_y, late_y, late_send, late_recv, y_peer)

    def add_late(j, _):
        k = late_chunk(j)
        put(k, block(k, own, z)[...] + late_y[j])
        return 0

    all_late().wait_recv()
    lax.fori_loop(0, lates, add_late, 0)
    lax.fori_loop(first_tail, chunks, finish_tail, None)

    totals = counted[...]
    for d in range(1, experts):
        sender = lax.rem(e + d, experts)
        count_copy(d, sender).wait_recv()
        totals = totals + seen[sender]
    for layer in range(layers):
        share = jnp.sum(jnp.sum(squares[layer], axis=0, keepdims=True), axis=1, keepdims=True)
        totals = jnp.where(row == layer, share, totals)
    message[...] = totals
    gathered[me] = totals

    def all_copy(d, sender):
        return remote(
            message, gathered.at[sender], all_send, all_recv, group_peer(d)[1]
        )

    for d in range(1, group):
        all_copy(d, me).start()
    def drain_rest(k, _):
        drain_z(k)
        sent(k, line, tail_send.at[k - first_tail])

    for k in range(chunks - min(SLOTS, chunks), chunks):
        core_copy(k).wait_send()
    lax.fori_loop(
        steps - behind, first_tail, lambda k, _: when_chain(k, drain_z), None
    )
    lax.fori_loop(first_tail, chunks, drain_rest, None)
    all_late().wait_send()

    def all_others():
        others = gathered.at[0:group - 1]
        return remote(others, others, all_send, all_recv, y_peer)

    all_others().wait_recv()
    total = gathered[0]
    for p in range(1, group):
        total = total + gathered[p]
    stats = jnp.zeros_like(total)
    for layer in range(layers):
        loads = total[layers + layer:layers + layer + 1, :]
        spot = lane[:1]
        own_load = jnp.sum(jnp.where(spot == e, loads, 0.0), axis=1, keepdims=True)
        mean_load = jnp.sum(jnp.where(spot < experts, loads, 0.0), axis=1, keepdims=True) / experts
        root_mean = jnp.sqrt(total[layer:layer + 1, :1] / numel)
        factor = (
            step_size * (own_load / mean_load) * clip_level / jnp.maximum(root_mean, clip_level)
        )
        beta = own_load / (own_load + mean_load)
        stats = jnp.where(row == layer, factor, stats)
        stats = jnp.where(row == layers + layer, beta, stats)
    stat_ref[...] = stats

    all_others().wait_send()
    for d in range(1, experts):
        count_copy(d, e).wait_send()


def update(
    layers, ff, stats, summed, weights, shadow, new_weights, new_shadow, updated, smoothed,
    weights_sem, shadow_sem,
):
    width = ff // SPLIT
    for layer in range(layers):
        factor = stats[layer:layer + 1, :1]
        beta = stats[layers + layer:layers + layer + 1, :1]
        for p in range(SPLIT):
            at = slice(p * width, (p + 1) * width)
            fresh = weights[layer, :, at] - factor * summed[layer, :, at]
            previous = shadow[layer, :, at]
            updated[layer, :, at] = fresh
            smoothed[layer, :, at] = previous + beta * (fresh - previous)
            pltpu.make_async_copy(
                updated.at[layer, :, at], new_weights.at[layer, :, at], weights_sem
            ).start()
            pltpu.make_async_copy(
                smoothed.at[layer, :, at], new_shadow.at[layer, :, at], shadow_sem
            ).start()
    pltpu.make_async_copy(updated, new_weights, weights_sem).wait()
    pltpu.make_async_copy(smoothed, new_shadow, shadow_sem).wait()


def on_device(sizes, activations, out_grads, weights, shadow, counts):
    line, experts, shards = sizes
    layers, _, tokens, all_rows = activations.shape
    ff, rows = out_grads.shape[3], weights.shape[2]
    assert shards == 2 * CORES and 2 * layers <= 8
    units = ff // 128
    per_layer = next(
        p for p in range(PIECES, units + 1) if units % p == 0 and units // p % 2 == 0
    )
    width = ff // per_layer
    chunks = layers * per_layer
    half = line * rows
    group = line * shards
    period = max(2, 2 * (line - 1))
    lates = chunks // period - FEWER
    period = max(2, period - CUT)
    ring = HOP * (line - 1) + HOP + 3
    y_ring = 2 * LAG + 2
    assert (lates - 1) * period + 1 < chunks - TAIL
    late_ring = min(lates, -(-(HOP_LATE * (line - 1) + HOP + 6) // period))
    f32 = jnp.float32
    dma = pltpu.SemaphoreType.DMA
    vmem = pl.BlockSpec(memory_space=pltpu.VMEM)
    hbm = pl.BlockSpec(memory_space=pltpu.HBM)
    dims = (
        line, experts, shards, layers, per_layer, width, rows, all_rows * ff, period, lates, ring,
        late_ring, y_ring,
    )
    summed, stats = pl.pallas_call(
        functools.partial(kernel, dims),
        out_shape=(
            jax.ShapeDtypeStruct((layers, rows, ff), f32), jax.ShapeDtypeStruct((8, 128), f32)
        ),
        in_specs=[hbm] * 3,
        out_specs=(vmem, vmem),
        scratch_shapes=[
            pltpu.VMEM((layers, tokens, all_rows), activations.dtype),
            pltpu.SMEM((layers, 1, experts), jnp.int32),
            pltpu.VMEM((CORES, 2 * half, tokens), f32),
            pltpu.VMEM((layers, CORES, 2 * half, tokens), activations.dtype),
            pltpu.VMEM((RING, tokens, width), out_grads.dtype),
            pltpu.VMEM((chunks, 2 * half, width), f32),
            pltpu.VMEM((chunks, half, width), f32),
            pltpu.VMEM((chunks, line + 1, rows, width), f32),
            pltpu.VMEM((lates, 2 * (line + 1), rows, width), f32),
            pltpu.VMEM((lates, rows, width), f32),
            pltpu.VMEM((SLOTS, 2 * half, width), f32),
            pltpu.VMEM((layers, rows, width), f32),
            pltpu.VMEM((8, 128), f32),
            pltpu.VMEM((experts, 8, 128), f32),
            pltpu.VMEM((8, 128), f32),
            pltpu.VMEM((group, 8, 128), f32),
            dma, dma, dma((RING,)),
            dma((SLOTS,)), dma((SLOTS,)), dma((y_ring,)), dma((y_ring,)),
            dma((TAIL,)), dma((TAIL, line)),
            dma((ring,)), dma((ring, line + 1)),
            dma((late_ring,)), dma((late_ring, 2 * (line + 1))),
            dma, dma, dma((experts,)), dma((experts,)), dma, dma,
        ],
        compiler_params=pltpu.CompilerParams(
            collective_id=0, has_side_effects=True, vmem_limit_bytes=46 * 1024 * 1024
        ),
        name="reduce_gradient",
    )(
        pltpu.with_memory_space_constraint(activations[:, 0], pltpu.HBM), out_grads[:, 0],
        pltpu.with_memory_space_constraint(counts, pltpu.HBM),
    )
    updated, smoothed = pl.pallas_call(
        functools.partial(update, layers, ff),
        out_shape=(jax.ShapeDtypeStruct((layers, rows, ff), f32),) * 2,
        in_specs=[vmem] * 4,
        out_specs=(hbm, hbm),
        scratch_shapes=[
            pltpu.VMEM((layers, rows, ff), f32), pltpu.VMEM((layers, rows, ff), f32), dma, dma
        ],
        compiler_params=pltpu.CompilerParams(vmem_limit_bytes=12 * 1024 * 1024),
        name="update",
    )(stats, summed, weights[:, 0], shadow[:, 0])
    return updated[:, None], smoothed[:, None]


def solution(mesh):
    rows = P(None, "expert", ("dp", "shard"), None)
    in_specs = (rows, rows, rows, rows, P(None, ("dp", "expert", "shard"), None))
    sizes = tuple(mesh.shape[a] for a in ("dp", "expert", "shard"))
    return jax.shard_map(
        functools.partial(on_device, sizes), mesh=mesh, in_specs=in_specs,
        out_specs=(rows, rows), check_vma=False,
    )
```

```python
import functools

import jax
import jax.numpy as jnp
from jax import lax
from jax.experimental import pallas as pl
from jax.experimental.pallas import tpu as pltpu
from jax.sharding import PartitionSpec as P

step_size = 0.5
clip_level = 1.0
CORES = 2
SLOTS = 4
LAG = 6
HOP = 3
HOP_LATE = 3
TAIL = 5
MID = 3
SPLIT = 4
AHEAD = 6
RING = 8
CUT = 0
FEWER = 0
PIECES = 28
MESH = pl.DeviceIdType.MESH


def kernel(
    dims, act_hbm, cot_hbm, cnt_hbm, out_ref, stat_ref,
    acts, cnt, turned, rows_ref, cot, merged, from_y, from_z, from_zx, late_y, staged,
    squares, counted, seen, message, gathered,
    act_sem, cnt_sem, cot_sem, core_send, core_recv, y_send, y_recv, tail_send, tail_recv, z_send, z_recv,
    zx_send, zx_recv, late_send, late_recv, cnt_send, cnt_recv, all_send, all_recv,
):
    line, experts, shards, layers, per_layer, width, rows, numel, period, lates, ring, late_ring, y_ring = dims
    group = line * shards
    half = line * rows
    chunks = layers * per_layer
    first_tail = chunks - TAIL
    first_mid = chunks - (MID if line > 3 else 0)
    z, e, s = lax.axis_index("dp"), lax.axis_index("expert"), lax.axis_index("shard")
    y, c = s // CORES, s % CORES
    me = z * shards + s
    core_peer = {"shard": y * CORES + (1 - c)}
    y_peer = {"shard": (1 - y) * CORES + c}
    own, other = y * half, (1 - y) * half

    def place(k):
        return k // per_layer, k % per_layer

    def columns(q):
        return pl.ds(pl.multiple_of(q * width, 128), width)

    def fetch(k):
        layer, q = place(k)
        return pltpu.make_async_copy(
            cot_hbm.at[layer, :, columns(q)], cot.at[k % RING], cot_sem.at[k % RING]
        )

    act_copy = pltpu.make_async_copy(act_hbm, acts, act_sem)
    cnt_fetch = pltpu.make_async_copy(cnt_hbm, cnt, cnt_sem)
    act_copy.start()
    fetch(0).start()

    def group_peer(d):
        p = lax.rem(me + d, group)
        return p, {"dp": p // shards, "shard": p % shards}

    def remote(src, dst, send, recv, device):
        return pltpu.make_async_remote_copy(
            src_ref=src, dst_ref=dst, send_sem=send, recv_sem=recv,
            device_id=device, device_id_type=MESH,
        )

    barrier = pltpu.get_barrier_semaphore()
    def greet(device):
        pl.semaphore_signal(barrier, inc=1, device_id=device, device_id_type=MESH)

    greet(core_peer)
    greet(y_peer)
    pl.when(z > 0)(lambda: greet({"dp": z - 1}))
    pl.when(z < line - 1)(lambda: greet({"dp": z + 1}))
    for d in range(1, experts):
        greet({"expert": lax.rem(e + d, experts)})
    for k in range(1, min(AHEAD, chunks)):
        fetch(k).start()
    cnt_fetch.start()

    def turn(layer):
        across = acts[layer].astype(jnp.float32).T
        for b in range(line):
            for h in range(shards // CORES):
                for core in range(CORES):
                    at = ((b * (shards // CORES) + h) * CORES + core) * rows
                    to = (h * line + b) * rows
                    turned[core, to:to + rows, :] = across[at:at + rows]
        for core in range(CORES):
            rows_ref[layer, core] = turned[core].astype(rows_ref.dtype)

    act_copy.wait()
    turn(0)
    ends = (z == 0).astype(jnp.int32) + (z == line - 1).astype(jnp.int32)
    pl.semaphore_wait(barrier, experts + 3 - ends)

    row = lax.broadcasted_iota(jnp.int32, counted.shape, 0)
    lane = lax.broadcasted_iota(jnp.int32, counted.shape, 1)

    def count_copy(d, sender):
        return remote(
            counted, seen.at[sender], cnt_send.at[d], cnt_recv.at[sender],
            {"expert": lax.rem(e + d, experts)},
        )

    def prepare():
        for layer in range(1, layers):
            turn(layer)
        cnt_fetch.wait()
        tile = jnp.zeros(counted.shape, jnp.float32)
        for layer in range(layers):
            for p in range(experts):
                here = (row == layers + layer) & (lane == p)
                tile = jnp.where(here, cnt[layer, 0, p].astype(jnp.float32), tile)
        counted[...] = tile
        squares[...] = jnp.zeros_like(squares)
        for d in range(1, experts):
            count_copy(d, e).start()

    def is_late(k):
        return (k % period == 1) & (k < period * lates)

    def late_chunk(j):
        return j * period + 1

    def when_chunk(k, body):
        pl.when((k >= 0) & (k < chunks))(lambda: body(k))

    def when_early(k, body):
        when_chunk(k, lambda k: pl.when(jnp.logical_not(is_late(k)))(lambda: body(k)))

    def when_chain(k, body):
        when_early(k, lambda k: pl.when(k < first_tail)(lambda: body(k)))

    def when_tail(k, body):
        pl.when((k >= first_tail) & (k < chunks))(lambda: body(k))

    def when_late(k, body):
        when_chunk(k, lambda k: pl.when(is_late(k))(lambda: body(k)))

    def core_copy(k):
        return remote(
            staged.at[k % SLOTS], merged.at[k], core_send.at[k % SLOTS], core_recv.at[k % SLOTS], core_peer
        )

    def y_copy(k):
        return remote(
            merged.at[k, pl.ds(pl.multiple_of(other, 8), half)], from_y.at[k],
            y_send.at[k % y_ring], y_recv.at[k % y_ring], y_peer,
        )

    def late_copy(k):
        j = k // period
        return remote(
            merged.at[k, pl.ds(pl.multiple_of(other + z * rows, 8), rows)], late_y.at[j],
            late_send, late_recv, y_peer,
        )

    def product(k, core):
        layer, _ = place(k)
        return jnp.dot(
            rows_ref[layer, core], cot[k % RING], preferred_element_type=jnp.float32
        )

    def stage_partner(k):
        pl.when(k >= SLOTS)(lambda: core_copy(k - SLOTS).wait_send())
        fetch(k).wait()
        staged[k % SLOTS] = product(k, 1 - c)
        core_copy(k).start()

    def merge_core(k):
        core_copy(k).wait_recv()
        merged[k] = merged[k] + product(k, c)
        when_chain(k, lambda k: y_copy(k).start())
        when_tail(k, lambda k: other_blocks(lambda b: tail_copy(k, b).start()))

    def tail_copy(k, b):
        i = k - first_tail
        at = pl.ds(pl.multiple_of(other + b * rows, 8), rows)
        return remote(
            merged.at[k, at], from_y.at[k, b * rows:(b + 1) * rows],
            tail_send.at[i], tail_recv.at[i, b], y_peer,
        )

    def other_blocks(body):
        for b in range(line):
            pl.when(z != b)(lambda: body(b))

    def own_block(body):
        for b in range(line):
            pl.when(z == b)(lambda: body(b))

    def merge_y(k):
        y_copy(k).wait_recv()
        at = pl.ds(pl.multiple_of(own, 8), half)
        merged[k, at, :] = merged[k, at, :] + from_y[k]

    def merge_block(k, b):
        tail_copy(k, b).wait_recv()
        at = pl.ds(pl.multiple_of(own + b * rows, 8), rows)
        merged[k, at, :] = merged[k, at, :] + from_y[k, b * rows:(b + 1) * rows, :]

    def merge_tail(k):
        other_blocks(lambda b: merge_block(k, b))

    def block(k, base, b):
        return merged.at[k, pl.ds(pl.multiple_of(base + b * rows, 8), rows)]

    def z_copy(k, base, b, slot, device, late):
        if late is None:
            return remote(
                block(k, base, b), from_z.at[k, slot], z_send.at[k % ring],
                z_recv.at[k % ring, slot], device,
            )
        j = k // period
        n = late * (line + 1) + slot
        return remote(
            block(k, base, b), from_zx.at[j, n], zx_send.at[j % late_ring],
            zx_recv.at[j % late_ring, n], device,
        )

    def arrived(k, slot, late):
        if late is None:
            return from_z[k, slot]
        return from_zx[k // period, late * (line + 1) + slot]

    def add_arrived(k, base, b, slot, late):
        z_copy(k, base, b, slot, {"dp": z}, late).wait_recv()
        ref = block(k, base, b)
        ref[...] = ref[...] + arrived(k, slot, late)

    def send_right(k, base, b, late):
        @pl.when(z < b)
        def _():
            pl.when(z > 0)(lambda: add_arrived(k, base, b, b + 1, late))
            z_copy(k, base, b, b + 1, {"dp": z + 1}, late).start()

    def send_left(k, base, b, late):
        @pl.when(z > b)
        def _():
            pl.when(z < line - 1)(lambda: add_arrived(k, base, b, b, late))
            z_copy(k, base, b, b, {"dp": z - 1}, late).start()

    def to_right(k, base, late):
        for b in reversed(range(1, line)):
            send_right(k, base, b, late)

    def to_left(k, base, late):
        for b in range(line - 1):
            send_left(k, base, b, late)

    def sooner(k, b, last):
        return k < first_mid if b == last and line > 3 else k >= 0

    def far_right(k):
        for b in reversed(range(2, line)):
            pl.when(sooner(k, b, 2))(lambda: send_right(k, own, b, None))

    def far_left(k):
        for b in range(line - 2):
            pl.when(sooner(k, b, line - 3))(lambda: send_left(k, own, b, None))

    def mid_right(k, _):
        send_right(k, own, 2, None)

    def mid_left(k, _):
        send_left(k, own, line - 3, None)

    def near_right(k, _):
        send_right(k, own, 1, None)

    def near_left(k, _):
        send_left(k, own, line - 2, None)

    def both_halves(one):
        def body(k):
            one(k, other, 0)
            one(k, own, 1)
        return body

    def own_half(one):
        return lambda k: one(k, own, None)

    def put(k, values):
        layer, q = place(k)
        out_ref[layer, :, columns(q)] = values
        squares[layer] = squares[layer] + values * values

    def gather_block(k, base, late):
        pl.when(z > 0)(lambda: add_arrived(k, base, z, z + 1, late))
        pl.when(z < line - 1)(lambda: add_arrived(k, base, z, z, late))

    def finish_early(k):
        gather_block(k, own, None)
        put(k, block(k, own, z)[...])

    def finish_tail(k, _):
        own_block(lambda b: merge_block(k, b))
        finish_early(k)

    def finish_late(k):
        gather_block(k, other, 0)
        gather_block(k, own, 1)

    back = line - 1 - z
    far = jnp.maximum(z, back)

    def on_tail(body):
        return lambda: lax.fori_loop(first_tail, chunks, body, None)

    def on_mid(body):
        return lambda: lax.fori_loop(first_mid, chunks, body, None)

    def step(t, _):
        pl.when(t + AHEAD < chunks)(lambda: fetch(t + AHEAD).start())
        when_chunk(t, stage_partner)
        when_chunk(t - 1, merge_core)
        when_late(t - 1 - HOP_LATE * z, both_halves(to_right))
        when_late(t - 1 - HOP_LATE * back, both_halves(to_left))
        when_late(t - 1 - HOP_LATE * far, finish_late)
        pl.when(t == 2)(prepare)
        when_chain(t - LAG, merge_y)
        when_tail(t - LAG, merge_tail)
        when_chain(t - LAG - HOP * z, own_half(to_right))
        when_chain(t - LAG - HOP * back, own_half(to_left))
        when_chain(t - LAG - HOP * far, finish_early)
        when_tail(t - LAG - HOP * z, far_right)
        when_tail(t - LAG - HOP * back, far_left)
        pl.when(t == chunks - 1 + LAG + HOP * z)(on_mid(mid_right))
        pl.when(t == chunks - 1 + LAG + HOP * back)(on_mid(mid_left))
        pl.when((t == chunks - 1 + LAG) & (z == 0))(on_tail(near_right))
        pl.when((t == chunks - 1 + LAG) & (back == 0))(on_tail(near_left))
        pl.when(t == start_late)(send_lates)
        when_chain(t - LAG - 1, drain_y)
        when_late(t - late_behind, drain_late)
        when_chain(t - behind, drain_z)
        return 0

    late_end = late_chunk(lates - 1) + 1 + HOP_LATE * (line - 1)
    start_late = max(chunks, late_end)
    behind = LAG + HOP * (line - 1) + 3
    late_behind = HOP_LATE * (line - 1) + 3
    steps = max(chunks + LAG + HOP * (line - 1), start_late + 1)

    def send_late(j, _):
        late_copy(late_chunk(j)).start()

    def send_own(k, _):
        own_block(lambda b: tail_copy(k, b).start())

    def send_lates():
        lax.fori_loop(0, lates, send_late, None)
        lax.fori_loop(first_tail, chunks, send_own, None)

    def drain_y(k):
        y_copy(k).wait_send()

    def sent(k, count, semaphore):
        ref = merged.at[k, 0:count * rows]
        remote(ref, ref, semaphore, semaphore, y_peer).wait_send()

    def drain_z(k):
        sent(k, line - 1, z_send.at[k % ring])

    def drain_late(k):
        sent(k, 2 * (line - 1), zx_send.at[k // period % late_ring])

    lax.fori_loop(0, steps, step, 0)

    def all_late():
        return remote(late_y, late_y, late_send, late_recv, y_peer)

    def add_late(j, _):
        k = late_chunk(j)
        put(k, block(k, own, z)[...] + late_y[j])
        return 0

    all_late().wait_recv()
    lax.fori_loop(0, lates, add_late, 0)
    lax.fori_loop(first_tail, chunks, finish_tail, None)

    totals = counted[...]
    for d in range(1, experts):
        sender = lax.rem(e + d, experts)
        count_copy(d, sender).wait_recv()
        totals = totals + seen[sender]
    for layer in range(layers):
        share = jnp.sum(jnp.sum(squares[layer], axis=0, keepdims=True), axis=1, keepdims=True)
        totals = jnp.where(row == layer, share, totals)
    message[...] = totals
    gathered[me] = totals

    def all_copy(d, sender):
        return remote(
            message, gathered.at[sender], all_send, all_recv, group_peer(d)[1]
        )

    for d in range(1, group):
        all_copy(d, me).start()
    def drain_rest(k, _):
        drain_z(k)
        sent(k, line, tail_send.at[k - first_tail])

    for k in range(chunks - min(SLOTS, chunks), chunks):
        core_copy(k).wait_send()
    lax.fori_loop(
        steps - behind, first_tail, lambda k, _: when_chain(k, drain_z), None
    )
    lax.fori_loop(first_tail, chunks, drain_rest, None)
    all_late().wait_send()

    def all_others():
        others = gathered.at[0:group - 1]
        return remote(others, others, all_send, all_recv, y_peer)

    all_others().wait_recv()
    total = gathered[0]
    for p in range(1, group):
        total = total + gathered[p]
    stats = jnp.zeros_like(total)
    for layer in range(layers):
        loads = total[layers + layer:layers + layer + 1, :]
        spot = lane[:1]
        own_load = jnp.sum(jnp.where(spot == e, loads, 0.0), axis=1, keepdims=True)
        mean_load = jnp.sum(jnp.where(spot < experts, loads, 0.0), axis=1, keepdims=True) / experts
        root_mean = jnp.sqrt(total[layer:layer + 1, :1] / numel)
        factor = (
            step_size * (own_load / mean_load) * clip_level / jnp.maximum(root_mean, clip_level)
        )
        beta = own_load / (own_load + mean_load)
        stats = jnp.where(row == layer, factor, stats)
        stats = jnp.where(row == layers + layer, beta, stats)
    stat_ref[...] = stats

    all_others().wait_send()
    for d in range(1, experts):
        count_copy(d, e).wait_send()


def update(
    layers, ff, stats, summed, weights, shadow, new_weights, new_shadow, updated, smoothed,
    weights_sem, shadow_sem,
):
    width = ff // SPLIT
    for layer in range(layers):
        factor = stats[layer:layer + 1, :1]
        beta = stats[layers + layer:layers + layer + 1, :1]
        for p in range(SPLIT):
            at = slice(p * width, (p + 1) * width)
            fresh = weights[layer, :, at] - factor * summed[layer, :, at]
            previous = shadow[layer, :, at]
            updated[layer, :, at] = fresh
            smoothed[layer, :, at] = previous + beta * (fresh - previous)
            pltpu.make_async_copy(
                updated.at[layer, :, at], new_weights.at[layer, :, at], weights_sem
            ).start()
            pltpu.make_async_copy(
                smoothed.at[layer, :, at], new_shadow.at[layer, :, at], shadow_sem
            ).start()
    pltpu.make_async_copy(updated, new_weights, weights_sem).wait()
    pltpu.make_async_copy(smoothed, new_shadow, shadow_sem).wait()


def on_device(sizes, activations, out_grads, weights, shadow, counts):
    line, experts, shards = sizes
    layers, _, tokens, all_rows = activations.shape
    ff, rows = out_grads.shape[3], weights.shape[2]
    assert shards == 2 * CORES and 2 * layers <= 8
    units = ff // 128
    per_layer = next(
        p for p in range(PIECES, units + 1) if units % p == 0 and units // p % 2 == 0
    )
    width = ff // per_layer
    chunks = layers * per_layer
    half = line * rows
    group = line * shards
    period = max(2, 2 * (line - 1))
    lates = chunks // period - FEWER
    period = max(2, period - CUT)
    ring = HOP * (line - 1) + HOP + 3
    y_ring = 2 * LAG + 2
    assert (lates - 1) * period + 1 < chunks - TAIL
    late_ring = min(lates, -(-(HOP_LATE * (line - 1) + HOP + 6) // period))
    f32 = jnp.float32
    dma = pltpu.SemaphoreType.DMA
    vmem = pl.BlockSpec(memory_space=pltpu.VMEM)
    hbm = pl.BlockSpec(memory_space=pltpu.HBM)
    dims = (
        line, experts, shards, layers, per_layer, width, rows, all_rows * ff, period, lates, ring,
        late_ring, y_ring,
    )
    summed, stats = pl.pallas_call(
        functools.partial(kernel, dims),
        out_shape=(
            jax.ShapeDtypeStruct((layers, rows, ff), f32), jax.ShapeDtypeStruct((8, 128), f32)
        ),
        in_specs=[hbm] * 3,
        out_specs=(vmem, vmem),
        scratch_shapes=[
            pltpu.VMEM((layers, tokens, all_rows), activations.dtype),
            pltpu.SMEM((layers, 1, experts), jnp.int32),
            pltpu.VMEM((CORES, 2 * half, tokens), f32),
            pltpu.VMEM((layers, CORES, 2 * half, tokens), activations.dtype),
            pltpu.VMEM((RING, tokens, width), out_grads.dtype),
            pltpu.VMEM((chunks, 2 * half, width), f32),
            pltpu.VMEM((chunks, half, width), f32),
            pltpu.VMEM((chunks, line + 1, rows, width), f32),
            pltpu.VMEM((lates, 2 * (line + 1), rows, width), f32),
            pltpu.VMEM((lates, rows, width), f32),
            pltpu.VMEM((SLOTS, 2 * half, width), f32),
            pltpu.VMEM((layers, rows, width), f32),
            pltpu.VMEM((8, 128), f32),
            pltpu.VMEM((experts, 8, 128), f32),
            pltpu.VMEM((8, 128), f32),
            pltpu.VMEM((group, 8, 128), f32),
            dma, dma, dma((RING,)),
            dma((SLOTS,)), dma((SLOTS,)), dma((y_ring,)), dma((y_ring,)),
            dma((TAIL,)), dma((TAIL, line)),
            dma((ring,)), dma((ring, line + 1)),
            dma((late_ring,)), dma((late_ring, 2 * (line + 1))),
            dma, dma, dma((experts,)), dma((experts,)), dma, dma,
        ],
        compiler_params=pltpu.CompilerParams(
            collective_id=0, has_side_effects=True, vmem_limit_bytes=46 * 1024 * 1024
        ),
        name="reduce_gradient",
    )(
        pltpu.with_memory_space_constraint(activations[:, 0], pltpu.HBM), out_grads[:, 0],
        pltpu.with_memory_space_constraint(counts, pltpu.HBM),
    )
    updated, smoothed = pl.pallas_call(
        functools.partial(update, layers, ff),
        out_shape=(jax.ShapeDtypeStruct((layers, rows, ff), f32),) * 2,
        in_specs=[vmem] * 4,
        out_specs=(hbm, hbm),
        scratch_shapes=[
            pltpu.VMEM((layers, rows, ff), f32), pltpu.VMEM((layers, rows, ff), f32), dma, dma
        ],
        compiler_params=pltpu.CompilerParams(vmem_limit_bytes=12 * 1024 * 1024),
        name="update",
    )(stats, summed, weights[:, 0], shadow[:, 0])
    return updated[:, None], smoothed[:, None]


def solution(mesh):
    rows = P(None, "expert", ("dp", "shard"), None)
    in_specs = (rows, rows, rows, rows, P(None, ("dp", "expert", "shard"), None))
    sizes = tuple(mesh.shape[a] for a in ("dp", "expert", "shard"))
    return jax.shard_map(
        functools.partial(on_device, sizes), mesh=mesh, in_specs=in_specs,
        out_specs=(rows, rows), check_vma=False,
    )
```
